8 devices in a mesh: fsdp: 8 (over z, y, x, core).
Axes of the slice: x: 2, y: 2, z: 1, core: 2. Of those that a mesh axis runs over, the one named last changes fastest.
Arguments:
- tok_ids: int32 [16384], P('fsdp')
- tok_labels: int32 [16384], P('fsdp')
- loss_mask: int32 [16384], P('fsdp')
- emb_table: bfloat16 [32768, 256], P('fsdp')
- gain_mlp: float32 [256], replicated
- gain_head: float32 [256], replicated
- w_gate: bfloat16 [256, 2048], P('fsdp')
- w_up: bfloat16 [256, 2048], P('fsdp')
- w_down: bfloat16 [2048, 256], P('fsdp')
Outputs:
- output 1: float32 [], replicated
- output 2: float32 [32768, 256], P('fsdp')
- output 3: float32 [256, 2048], P('fsdp')
- output 4: float32 [256, 2048], P('fsdp')
- output 5: float32 [2048, 256], P('fsdp')
All inputs are finite; a program needn't handle non-finite values.
Results may differ from the reference program's by a relative error of at most 0.00867396.
Values are sent between devices in bfloat16 or wider.
A program may use at most 1 GiB of HBM per device.

```python
import jax
import jax.numpy as jnp
from jax import lax

VOCAB = 32768
D_MODEL = 256
D_FF = 2048
TOK_DEV = 2048
GROUP_SIZE = 8
T_GLOBAL = TOK_DEV * GROUP_SIZE
NORM_EPS = 1e-6
ROW_CONTRACT = (((1,), (1,)), ((), ()))
TOK_CONTRACT = (((0,), (0,)), ((), ()))


def draw_tokens(tok_key):
    key_ids, key_lab, key_pad, key_cut = jax.random.split(tok_key, 4)
    tok_ids = jax.random.randint(key_ids, (T_GLOBAL,), 0, VOCAB, dtype=jnp.int32)
    tok_ids = tok_ids.at[0].set(0).at[1].set(VOCAB - 1)
    tok_labels = jax.random.randint(key_lab, (T_GLOBAL,), 0, VOCAB, dtype=jnp.int32)
    tok_labels = tok_labels.at[0].set(VOCAB - 1).at[1].set(0)
    pad_len = jax.random.randint(key_pad, (GROUP_SIZE, 1), 0, TOK_DEV // 2 + 1, dtype=jnp.int32)
    keep_tail = jnp.arange(TOK_DEV)[None, :] < TOK_DEV - pad_len
    cut_draw = jax.random.randint(key_cut, (GROUP_SIZE, TOK_DEV), 0, 16, dtype=jnp.int32)
    loss_mask = (keep_tail & (cut_draw != 0)).astype(jnp.int32).reshape(T_GLOBAL)
    return tok_ids, tok_labels, loss_mask.at[0].set(1)


def setup_inputs(seed: int = 0) -> dict:
    root_key = jax.random.key(seed)
    key_tok, key_emb, key_g1, key_g2, key_gate, key_up, key_down = jax.random.split(root_key, 7)
    tok_ids, tok_labels, loss_mask = draw_tokens(key_tok)
    emb_table = (jax.random.normal(key_emb, (VOCAB, D_MODEL), jnp.float32) * D_MODEL ** -0.5).astype(jnp.bfloat16)
    gain_mlp = 1.0 + 0.5 * jax.random.normal(key_g1, (D_MODEL,), jnp.float32)
    gain_head = 1.0 + 0.5 * jax.random.normal(key_g2, (D_MODEL,), jnp.float32)
    w_gate = (jax.random.normal(key_gate, (D_MODEL, D_FF), jnp.float32) * D_MODEL ** -0.5).astype(jnp.bfloat16)
    w_up = (jax.random.normal(key_up, (D_MODEL, D_FF), jnp.float32) * D_MODEL ** -0.5).astype(jnp.bfloat16)
    w_down = (jax.random.normal(key_down, (D_FF, D_MODEL), jnp.float32) * 1.5 * (D_FF * D_MODEL) ** -0.5).astype(jnp.bfloat16)
    return {"tok_ids": tok_ids, "tok_labels": tok_labels, "loss_mask": loss_mask, "emb_table": emb_table, "gain_mlp": gain_mlp, "gain_head": gain_head, "w_gate": w_gate, "w_up": w_up, "w_down": w_down}


def rms_scale(rows_wide, norm_gain):
    inv_rms = lax.rsqrt(jnp.mean(rows_wide * rows_wide, axis=-1, keepdims=True) + NORM_EPS)
    return (rows_wide * inv_rms * norm_gain).astype(jnp.bfloat16), inv_rms


def rms_back(rows_wide, inv_rms, norm_gain, grad_out):
    scaled_grad = grad_out * norm_gain
    return inv_rms * (scaled_grad - rows_wide * (inv_rms * inv_rms) * jnp.mean(scaled_grad * rows_wide, axis=-1, keepdims=True))


def mlp_forward(emb_rows, gain_mlp, gain_head, w_gate, w_up, w_down):
    emb_wide = emb_rows.astype(jnp.float32)
    a_norm, inv_first = rms_scale(emb_wide, gain_mlp)
    gate_wide = jnp.dot(a_norm, w_gate, preferred_element_type=jnp.float32).astype(jnp.bfloat16).astype(jnp.float32)
    up_wide = jnp.dot(a_norm, w_up, preferred_element_type=jnp.float32).astype(jnp.bfloat16).astype(jnp.float32)
    gate_sig = jax.nn.sigmoid(gate_wide)
    act_rows = (gate_wide * gate_sig * up_wide).astype(jnp.bfloat16)
    hid_wide = (emb_wide + jnp.dot(act_rows, w_down, preferred_element_type=jnp.float32)).astype(jnp.bfloat16).astype(jnp.float32)
    h_norm, inv_second = rms_scale(hid_wide, gain_head)
    return (emb_wide, inv_first, a_norm, gate_wide, up_wide, gate_sig, act_rows, hid_wide, inv_second), h_norm


def head_forward(h_norm, emb_table, tok_labels, tok_coef):
    logits = lax.dot_general(h_norm, emb_table, ROW_CONTRACT, preferred_element_type=jnp.float32)
    row_max = jnp.max(logits, axis=-1, keepdims=True)
    exp_rows = jnp.exp(logits - row_max)
    sum_exp = jnp.sum(exp_rows, axis=-1, keepdims=True)
    is_label = jnp.arange(logits.shape[1])[None, :] == tok_labels[:, None]
    picked = jnp.sum(jnp.where(is_label, logits, 0.0), axis=-1)
    tok_loss = row_max[:, 0] + jnp.log(sum_exp[:, 0]) - picked
    d_logits = ((exp_rows / sum_exp - is_label.astype(jnp.float32)) * tok_coef[:, None]).astype(jnp.bfloat16)
    return jnp.sum(tok_coef * tok_loss), d_logits


def mlp_backward(saved, d_hidden, gain_mlp, w_gate, w_up, w_down):
    emb_wide, inv_first, a_norm, gate_wide, up_wide, gate_sig, act_rows = saved[:7]
    hid_grad = d_hidden.astype(jnp.bfloat16)
    d_act = lax.dot_general(hid_grad, w_down, ROW_CONTRACT, preferred_element_type=jnp.float32)
    grad_down = lax.dot_general(act_rows, hid_grad, TOK_CONTRACT, preferred_element_type=jnp.float32)
    d_up = (d_act * gate_wide * gate_sig).astype(jnp.bfloat16)
    d_gate = (d_act * up_wide * gate_sig * (1.0 + gate_wide * (1.0 - gate_sig))).astype(jnp.bfloat16)
    grad_gate = lax.dot_general(a_norm, d_gate, TOK_CONTRACT, preferred_element_type=jnp.float32)
    grad_up = lax.dot_general(a_norm, d_up, TOK_CONTRACT, preferred_element_type=jnp.float32)
    d_anorm = lax.dot_general(d_gate, w_gate, ROW_CONTRACT, preferred_element_type=jnp.float32) + lax.dot_general(d_up, w_up, ROW_CONTRACT, preferred_element_type=jnp.float32)
    grad_x = d_hidden + rms_back(emb_wide, inv_first, gain_mlp, d_anorm)
    return grad_x, grad_gate, grad_up, grad_down


def block_grads(tok_ids, tok_labels, tok_coef, emb_table, gain_mlp, gain_head, w_gate, w_up, w_down):
    saved, h_norm = mlp_forward(jnp.take(emb_table, tok_ids, axis=0), gain_mlp, gain_head, w_gate, w_up, w_down)
    loss_part, d_logits = head_forward(h_norm, emb_table, tok_labels, tok_coef)
    d_hnorm = jnp.dot(d_logits, emb_table, preferred_element_type=jnp.float32)
    head_grad = lax.dot_general(d_logits, h_norm, TOK_CONTRACT, preferred_element_type=jnp.float32)
    d_hidden = rms_back(saved[7], saved[8], gain_head, d_hnorm)
    grad_x, grad_gate, grad_up, grad_down = mlp_backward(saved, d_hidden, gain_mlp, w_gate, w_up, w_down)
    grad_table = head_grad + jax.ops.segment_sum(grad_x, tok_ids, num_segments=emb_table.shape[0])
    return loss_part, grad_table, grad_gate, grad_up, grad_down


def reference(tok_ids, tok_labels, loss_mask, emb_table, gain_mlp, gain_head, w_gate, w_up, w_down):
    mask_wide = loss_mask.astype(jnp.float32)
    tok_coef = (mask_wide / jnp.sum(mask_wide)).reshape(GROUP_SIZE, TOK_DEV)

    def scan_step(acc_state, block_in):
        step_out = block_grads(block_in[0], block_in[1], block_in[2], emb_table, gain_mlp, gain_head, w_gate, w_up, w_down)
        return tuple(prev_val + new_val for prev_val, new_val in zip(acc_state, step_out)), None

    init_state = (jnp.zeros((), jnp.float32), jnp.zeros((VOCAB, D_MODEL), jnp.float32), jnp.zeros((D_MODEL, D_FF), jnp.float32), jnp.zeros((D_MODEL, D_FF), jnp.float32), jnp.zeros((D_FF, D_MODEL), jnp.float32))
    blocks = (tok_ids.reshape(GROUP_SIZE, TOK_DEV), tok_labels.reshape(GROUP_SIZE, TOK_DEV), tok_coef)
    final_state, _ = lax.scan(scan_step, init_state, blocks)
    loss_val, grad_table, grad_gate, grad_up, grad_down = final_state
    return (loss_val, grad_table, grad_gate, grad_up, grad_down)
```

```python
import functools
import math

import jax
import jax.numpy as jnp
from jax import lax
from jax.experimental import pallas as pl
from jax.experimental.pallas import tpu as pltpu
from jax.sharding import PartitionSpec as P

NORM_EPS = 1e-6
ROW_CONTRACT = (((1,), (1,)), ((), ()))
TOK_CONTRACT = (((0,), (0,)), ((), ()))
MESH = pl.DeviceIdType.MESH
LOG2E = math.log2(math.e)
LN2 = math.log(2.0)
N_DEV = 8
UNIT = 256
V_CHUNK = 512
VMEM_MAX = 67_043_328


def peer_of(me, step):
    core = (me % 2 + step % 2) % 2
    col = ((me // 2) % 2 + (step // 2) % 2) % 2
    row = (me // 4 + step // 4) % 2
    return row * 4 + col * 2 + core


def pair_xor(pair, other):
    return ((pair // 2 + other // 2) % 2) * 2 + (pair % 2 + other % 2) % 2


def meet_all(me):
    barrier = pltpu.get_barrier_semaphore()
    for step in range(1, N_DEV):
        pl.semaphore_signal(barrier, inc=1, device_id=(peer_of(me, step),), device_id_type=MESH)
    pl.semaphore_wait(barrier, N_DEV - 1)


def remote(src, dst, send_sem, recv_sem, target):
    return pltpu.make_async_remote_copy(src_ref=src, dst_ref=dst, send_sem=send_sem, recv_sem=recv_sem, device_id=(target,), device_id_type=MESH)


def tokens_kernel(tok_hbm, all_ref, local_sem, send_sems, recv_sems):
    me = lax.axis_index("fsdp")
    own = pltpu.make_async_copy(tok_hbm, all_ref.at[0], local_sem)
    own.start()
    meet_all(me)
    own.wait()
    copies = []
    for step in range(1, N_DEV):
        copy = remote(all_ref.at[0], all_ref.at[step], send_sems.at[step], recv_sems.at[step], peer_of(me, step))
        copy.start()
        copies.append(copy)
    for copy in copies:
        copy.wait()


def gather_tokens(tok_block):
    return pl.pallas_call(
        tokens_kernel,
        out_shape=jax.ShapeDtypeStruct((N_DEV,) + tok_block.shape, tok_block.dtype),
        in_specs=[pl.BlockSpec(memory_space=pl.ANY)],
        out_specs=pl.BlockSpec(memory_space=pltpu.VMEM),
        scratch_shapes=[pltpu.SemaphoreType.DMA, pltpu.SemaphoreType.DMA((N_DEV,)), pltpu.SemaphoreType.DMA((N_DEV,))],
        compiler_params=pltpu.CompilerParams(collective_id=0, has_side_effects=True),
        name="gather_tokens",
    )(tok_block)


def head_kernel(groups, vocab, hn_hbm, lab_hbm, norm_ref, table_ref, table_t_ref, dhn_ref, dtable_ref, lse_ref, pick_ref,
                hn_all, lab_all, lse_mine, lse_all, part_own, part_out, part_in, sum_in, dhn_acc,
                local_sems, ag_send, ag_recv, fw_send, lab_send, lab_recv, st_send, st_recv, d2_send, d2_recv, rs_send, rs_recv):
    me = lax.axis_index("fsdp")
    chunks = vocab // V_CHUNK
    pair_rows = 2 * UNIT

    lab_copy = pltpu.make_async_copy(lab_hbm, lab_all.at[0], local_sems.at[0])
    lab_copy.start()
    hn_copy = pltpu.make_async_copy(hn_hbm, hn_all.at[:, 0], local_sems.at[1])
    hn_copy.start()
    meet_all(me)
    lab_copy.wait()

    def label_send(step):
        return remote(lab_all.at[0], lab_all.at[step], lab_send.at[step], lab_recv.at[step], peer_of(me, step))

    def own_send(step, group):
        return remote(hn_all.at[group, 0], hn_all.at[group, step], ag_send.at[step, group], ag_recv.at[step, group], peer_of(me, step))

    def forward(step, group):
        return remote(hn_all.at[group, step], hn_all.at[group, step + 1], fw_send.at[step, group], ag_recv.at[step + 1, group], peer_of(me, 1))

    def stat_send(step, group):
        return remote(lse_mine.at[group], lse_all.at[group, step], st_send.at[step, group], st_recv.at[step, group], peer_of(me, step))

    def part_send(group, pair):
        return remote(part_out.at[group, pair], part_in.at[group, pair], d2_send.at[group, pair], d2_recv.at[group, pair], peer_of(me, 1))

    def home_send(group, pair):
        return remote(part_own.at[group, pair], sum_in.at[group, pair], rs_send.at[group, pair], rs_recv.at[group, pair], peer_of(me, 2 * pair))

    hn_copy.wait()

    @pl.loop(0, groups)
    def _(group):
        for step in (1, 2, 4, 6):
            own_send(step, group).start()

    for step in range(1, N_DEV):
        label_send(step).start()
    dtable_ref[...] = jnp.zeros_like(dtable_ref)
    pick_ref[...] = jnp.zeros_like(pick_ref)

    def table_rows(chunk):
        return table_ref[pl.ds(pl.multiple_of(chunk * V_CHUNK, V_CHUNK), V_CHUNK), :]

    @pl.loop(0, groups)
    def _(group):
        @pl.loop(0, 4)
        def _(pair):
            @pl.when(pair > 0)
            def _():
                own_send(2 * pair, group).wait_recv()
                forward(2 * pair, group).start()

            @pl.when(pair == 0)
            def _():
                own_send(1, group).wait_recv()

            @pl.when(pair > 0)
            def _():
                forward(2 * pair, group).wait_recv()

            tile = hn_all[group, pl.ds(2 * pair, 2)].reshape(pair_rows, 256)
            run_max = jnp.full((8, pair_rows), -jnp.inf, jnp.float32)
            run_sum = jnp.zeros((8, pair_rows), jnp.float32)
            for chunk in range(chunks):
                logits = lax.dot_general(table_rows(chunk), tile, ROW_CONTRACT, preferred_element_type=jnp.float32)
                logits = logits.reshape(V_CHUNK // 8, 8, pair_rows)
                new_max = jnp.maximum(run_max, jnp.max(logits, axis=0))
                new_scaled = new_max * LOG2E
                run_sum = run_sum * jnp.exp2(run_max * LOG2E - new_scaled) + jnp.sum(jnp.exp2(logits * LOG2E - new_scaled[None]), axis=0)
                run_max = new_max
            scaled = run_max * LOG2E
            top = jnp.max(scaled, axis=0, keepdims=True)
            total = jnp.sum(run_sum * jnp.exp2(scaled - top), axis=0, keepdims=True)
            lse_mine[group, pair] = top + jnp.log2(total)

        @pl.when(group > 0)
        def _():
            for step in range(1, N_DEV):
                stat_send(step, group - 1).start()

    for step in range(1, N_DEV):
        label_send(step).wait_recv()

    log2_n = norm_ref[0:1, :]
    log2_n = jnp.concatenate([log2_n] * (pair_rows // 128), axis=1)
    inv_n = norm_ref[1:2, :]
    inv_n = jnp.concatenate([inv_n] * (pair_rows // 128), axis=1)
    row_iota = lax.broadcasted_iota(jnp.int32, (V_CHUNK, pair_rows), 0)

    def finish_pair(group, pair):
        part_send(group, pair).wait_recv()
        part_own[group, pair] = part_own[group, pair] + part_in[group, pair]

    @pl.loop(0, groups)
    def _(group):
        @pl.when(group == 0)
        def _():
            for step in range(1, N_DEV):
                stat_send(step, groups - 1).start()

        for step in range(1, N_DEV):
            stat_send(step, group).wait_recv()

        @pl.loop(0, 4)
        def _(turn):
            pair = 3 - turn
            low, high = [], []
            for step in range(N_DEV):
                source = lse_mine.at[group] if step == 0 else lse_all.at[group, step]
                row = source[pair_xor(pair, step // 2)]
                halves = [row[:, :UNIT], row[:, UNIT:]]
                low.append(halves[step % 2])
                high.append(halves[1 - step % 2])
            both = [jnp.concatenate(two, axis=1) for two in zip(low, high)]
            top = functools.reduce(jnp.maximum, both)
            lse = top + jnp.log2(sum(jnp.exp2(part - top) for part in both))
            label = jnp.concatenate([lab_all[2 * pair, group], lab_all[2 * pair + 1, group]], axis=1)
            valid = label >= 0
            shift = jnp.where(valid, lse + log2_n, 1e30)

            @pl.when(pair == 0)
            def _():
                lse_ref[group] = jnp.where(valid, lse, 0.0)[:, :UNIT]

            tile = hn_all[group, pl.ds(2 * pair, 2)].reshape(pair_rows, 256)
            local_label = label - me * vocab
            picked = jnp.zeros((8, pair_rows), jnp.float32)
            for chunk in range(chunks):
                logits = lax.dot_general(table_rows(chunk), tile, ROW_CONTRACT, preferred_element_type=jnp.float32)
                is_label = row_iota == (local_label - chunk * V_CHUNK)
                picked += jnp.sum(jnp.where(is_label, logits, 0.0).reshape(V_CHUNK // 8, 8, pair_rows), axis=0)
                prob = jnp.exp2(logits * LOG2E - shift)
                d_logits = jnp.where(is_label, prob - inv_n, prob).astype(jnp.bfloat16)
                rows = pl.ds(chunk * V_CHUNK, V_CHUNK)
                dtable_ref[rows, :] += jnp.dot(d_logits, tile, preferred_element_type=jnp.float32)
                d_part = jnp.dot(table_t_ref[:, rows], d_logits, preferred_element_type=jnp.float32)
                if chunk == 0:
                    dhn_acc[...] = d_part
                else:
                    dhn_acc[...] += d_part
            pick_ref[...] += picked
            part_own[group, pair] = dhn_acc[:, :UNIT]
            part_out[group, pair] = dhn_acc[:, UNIT:]
            part_send(group, pair).start()

            @pl.when(turn > 0)
            def _():
                finish_pair(group, pair + 1)
                home_send(group, pair + 1).start()

            @pl.when((turn == 0) & (group > 0))
            def _():
                finish_pair(group - 1, 0)

    finish_pair(groups - 1, 0)

    @pl.loop(0, groups)
    def _(group):
        total = part_own[group, 0]
        for pair in (1, 2, 3):
            home_send(group, pair).wait_recv()
            total = total + sum_in[group, pair]
        dhn_ref[group] = total.T
        for step in (1, 2, 4, 6):
            own_send(step, group).wait_send()
        for step in (2, 4, 6):
            forward(step, group).wait_send()
        for step in range(1, N_DEV):
            stat_send(step, group).wait_send()
        for pair in range(4):
            part_send(group, pair).wait_send()
        for pair in (1, 2, 3):
            home_send(group, pair).wait_send()

    for step in range(1, N_DEV):
        label_send(step).wait_send()


def head_call(h_norm, labels, norm_rows, table, table_t, groups):
    vocab = table.shape[0]
    dma = pltpu.SemaphoreType.DMA
    vmem = pl.BlockSpec(memory_space=pltpu.VMEM)
    hbm = pl.BlockSpec(memory_space=pl.ANY)
    f32, bf16 = jnp.float32, jnp.bfloat16
    tokens = N_DEV * groups * UNIT
    return pl.pallas_call(
        functools.partial(head_kernel, groups, vocab),
        out_shape=(
            jax.ShapeDtypeStruct((groups, UNIT, 256), f32),
            jax.ShapeDtypeStruct((vocab, 256), f32),
            jax.ShapeDtypeStruct((groups, 1, UNIT), f32),
            jax.ShapeDtypeStruct((8, 2 * UNIT), f32),
        ),
        in_specs=[hbm, hbm, vmem, vmem, vmem],
        out_specs=(vmem, vmem, vmem, vmem),
        scratch_shapes=[
            pltpu.VMEM((groups, N_DEV, UNIT, 256), bf16),
            pltpu.VMEM((N_DEV, groups, 1, UNIT), jnp.int32),
            pltpu.VMEM((groups, 4, 1, 2 * UNIT), f32),
            pltpu.VMEM((groups, N_DEV, 4, 1, 2 * UNIT), f32),
            pltpu.VMEM((groups, 4, 256, UNIT), f32),
            pltpu.VMEM((groups, 4, 256, UNIT), f32),
            pltpu.VMEM((groups, 4, 256, UNIT), f32),
            pltpu.VMEM((groups, 4, 256, UNIT), f32),
            pltpu.VMEM((256, 2 * UNIT), f32),
            dma((2,)),
            dma((N_DEV, groups)),
            dma((N_DEV, groups)),
            dma((N_DEV, groups)),
            dma((N_DEV,)),
            dma((N_DEV,)),
            dma((N_DEV, groups)),
            dma((N_DEV, groups)),
            dma((groups, 4)),
            dma((groups, 4)),
            dma((groups, 4)),
            dma((groups, 4)),
        ],
        compiler_params=pltpu.CompilerParams(collective_id=1, has_side_effects=True, vmem_limit_bytes=VMEM_MAX),
        cost_estimate=pl.CostEstimate(flops=8 * tokens * vocab * 256, bytes_accessed=16 * vocab * 256, transcendentals=2 * tokens * vocab),
        name="head",
    )(h_norm, labels, norm_rows, table, table_t)


def rms_scale(rows_wide, norm_gain):
    inv_rms = lax.rsqrt(jnp.mean(rows_wide * rows_wide, axis=-1, keepdims=True) + NORM_EPS)
    return (rows_wide * inv_rms * norm_gain).astype(jnp.bfloat16), inv_rms


def rms_back(rows_wide, inv_rms, norm_gain, grad_out):
    scaled_grad = grad_out * norm_gain
    return inv_rms * (scaled_grad - rows_wide * (inv_rms * inv_rms) * jnp.mean(scaled_grad * rows_wide, axis=-1, keepdims=True))


def mlp_forward(emb_rows, gain_mlp, gain_head, w_gate, w_up, w_down):
    emb_wide = emb_rows.astype(jnp.float32)
    a_norm, inv_first = rms_scale(emb_wide, gain_mlp)
    gate_wide = jnp.dot(a_norm, w_gate, preferred_element_type=jnp.float32).astype(jnp.bfloat16).astype(jnp.float32)
    up_wide = jnp.dot(a_norm, w_up, preferred_element_type=jnp.float32).astype(jnp.bfloat16).astype(jnp.float32)
    gate_sig = jax.nn.sigmoid(gate_wide)
    act_rows = (gate_wide * gate_sig * up_wide).astype(jnp.bfloat16)
    hid_wide = (emb_wide + jnp.dot(act_rows, w_down, preferred_element_type=jnp.float32)).astype(jnp.bfloat16).astype(jnp.float32)
    h_norm, inv_second = rms_scale(hid_wide, gain_head)
    return (emb_wide, inv_first, a_norm, gate_wide, up_wide, gate_sig, act_rows, hid_wide, inv_second), h_norm


def mlp_backward(saved, d_hidden, gain_mlp, w_gate, w_up, w_down):
    emb_wide, inv_first, a_norm, gate_wide, up_wide, gate_sig, act_rows = saved[:7]
    hid_grad = d_hidden.astype(jnp.bfloat16)
    d_act = lax.dot_general(hid_grad, w_down, ROW_CONTRACT, preferred_element_type=jnp.float32)
    grad_down = lax.dot_general(act_rows, hid_grad, TOK_CONTRACT, preferred_element_type=jnp.float32)
    d_up = (d_act * gate_wide * gate_sig).astype(jnp.bfloat16)
    d_gate = (d_act * up_wide * gate_sig * (1.0 + gate_wide * (1.0 - gate_sig))).astype(jnp.bfloat16)
    grad_gate = lax.dot_general(a_norm, d_gate, TOK_CONTRACT, preferred_element_type=jnp.float32)
    grad_up = lax.dot_general(a_norm, d_up, TOK_CONTRACT, preferred_element_type=jnp.float32)
    d_anorm = lax.dot_general(d_gate, w_gate, ROW_CONTRACT, preferred_element_type=jnp.float32) + lax.dot_general(d_up, w_up, ROW_CONTRACT, preferred_element_type=jnp.float32)
    grad_x = d_hidden + rms_back(emb_wide, inv_first, gain_mlp, d_anorm)
    return grad_x, grad_gate, grad_up, grad_down


GROUPS = 7


def solution(mesh):
    def gather_rows(row_shard):
        return lax.all_gather(row_shard, "fsdp", axis=0, tiled=True)

    def scatter_rows(full_rows):
        return lax.psum_scatter(full_rows, "fsdp", scatter_dimension=0, tiled=True)

    def device_step(tok_ids, tok_labels, loss_mask, table_shard, gain_mlp, gain_head, gate_shard, up_shard, down_shard):
        me = lax.axis_index("fsdp")
        vocab, width = table_shard.shape
        vocab_all = vocab * N_DEV
        slots = GROUPS * UNIT
        gate_full, up_full, down_full = gather_rows(gate_shard), gather_rows(up_shard), gather_rows(down_shard)
        block = jnp.stack([tok_ids.reshape(-1, 128), tok_labels.reshape(-1, 128), loss_mask.reshape(-1, 128)])
        every = gather_tokens(block)
        ids, labels, mask = every[:, 0].reshape(-1), every[:, 1].reshape(-1), every[:, 2].reshape(-1)
        count = jnp.sum(mask).astype(jnp.float32)
        owner = ids // vocab
        loads = [jnp.sum(jnp.where(owner == dev, mask, 0)) for dev in range(N_DEV)]
        rounds = (functools.reduce(jnp.maximum, loads) + slots - 1) // slots
        last = jnp.int32(2**31 - 1)
        packed = jnp.where((owner == me) & (mask != 0), (ids - me * vocab) * vocab_all + labels, last)
        packed = jnp.sort(packed)
        most = -(-ids.shape[0] // slots) * slots
        packed = jnp.concatenate([packed, jnp.full((most - ids.shape[0],), last)])
        norm_rows = jnp.zeros((8, 128), jnp.float32).at[0].set(jnp.log2(count)).at[1].set(1.0 / count)
        table_t = table_shard.T

        def one_round(state):
            turn, loss, g_table, g_gate, g_up, g_down = state
            mine = lax.dynamic_slice(packed, (turn * slots,), (slots,))
            valid = mine != last
            row_id = jnp.where(valid, mine // vocab_all, 0)
            label = jnp.where(valid, mine % vocab_all, -1)
            saved, h_norm = mlp_forward(jnp.take(table_shard, row_id, axis=0), gain_mlp, gain_head, gate_full, up_full, down_full)
            d_hnorm, head_grad, lse, picked = head_call(h_norm.reshape(GROUPS, UNIT, width), label.reshape(GROUPS, 1, UNIT), norm_rows, table_shard, table_t, GROUPS)
            d_hidden = rms_back(saved[7], saved[8], gain_head, d_hnorm.reshape(slots, width))
            grad_x, grad_gate, grad_up, grad_down = mlp_backward(saved, d_hidden, gain_mlp, gate_full, up_full, down_full)
            in_grad = jax.ops.segment_sum(grad_x, row_id, num_segments=vocab)
            part = (jnp.sum(lse) * LN2 - jnp.sum(picked)) / count
            return (turn + 1, loss + part, g_table + head_grad + in_grad, g_gate + grad_gate, g_up + grad_up, g_down + grad_down)

        zeros = (jnp.int32(0), jnp.float32(0), jnp.zeros((vocab, width), jnp.float32), jnp.zeros(gate_full.shape, jnp.float32), jnp.zeros(up_full.shape, jnp.float32), jnp.zeros(down_full.shape, jnp.float32))
        _, loss, g_table, g_gate, g_up, g_down = lax.while_loop(lambda state: state[0] < rounds, one_round, zeros)
        return (lax.psum(loss, "fsdp"), g_table, scatter_rows(g_gate), scatter_rows(g_up), scatter_rows(g_down))

    row_spec = P("fsdp", None)
    tok_spec = P("fsdp")
    return jax.shard_map(device_step, mesh=mesh, in_specs=(tok_spec, tok_spec, tok_spec, row_spec, P(), P(), row_spec, row_spec, row_spec), out_specs=(P(), row_spec, row_spec, row_spec, row_spec), check_vma=False)
```

```python
import functools
import math

import jax
import jax.numpy as jnp
from jax import lax
from jax.experimental import pallas as pl
from jax.experimental.pallas import tpu as pltpu
from jax.sharding import PartitionSpec as P

NORM_EPS = 1e-6
ROW_CONTRACT = (((1,), (1,)), ((), ()))
TOK_CONTRACT = (((0,), (0,)), ((), ()))
MESH = pl.DeviceIdType.MESH
LOG2E = math.log2(math.e)
LN2 = math.log(2.0)
N_DEV = 8
UNIT = 256
V_CHUNK = 512
VMEM_MAX = 67_043_328


def peer_of(me, step):
    core = (me % 2 + step % 2) % 2
    col = ((me // 2) % 2 + (step // 2) % 2) % 2
    row = (me // 4 + step // 4) % 2
    return row * 4 + col * 2 + core


def pair_xor(pair, other):
    return ((pair // 2 + other // 2) % 2) * 2 + (pair % 2 + other % 2) % 2


def meet_all(me):
    barrier = pltpu.get_barrier_semaphore()
    for step in range(1, N_DEV):
        pl.semaphore_signal(barrier, inc=1, device_id=(peer_of(me, step),), device_id_type=MESH)
    pl.semaphore_wait(barrier, N_DEV - 1)


def remote(src, dst, send_sem, recv_sem, target):
    return pltpu.make_async_remote_copy(src_ref=src, dst_ref=dst, send_sem=send_sem, recv_sem=recv_sem, device_id=(target,), device_id_type=MESH)


def tokens_kernel(tok_hbm, all_ref, local_sem, send_sems, recv_sems):
    me = lax.axis_index("fsdp")
    own = pltpu.make_async_copy(tok_hbm, all_ref.at[0], local_sem)
    own.start()
    meet_all(me)
    own.wait()
    copies = []
    for step in range(1, N_DEV):
        copy = remote(all_ref.at[0], all_ref.at[step], send_sems.at[step], recv_sems.at[step], peer_of(me, step))
        copy.start()
        copies.append(copy)
    for copy in copies:
        copy.wait()


def gather_tokens(tok_block):
    return pl.pallas_call(
        tokens_kernel,
        out_shape=jax.ShapeDtypeStruct((N_DEV,) + tok_block.shape, tok_block.dtype),
        in_specs=[pl.BlockSpec(memory_space=pl.ANY)],
        out_specs=pl.BlockSpec(memory_space=pltpu.VMEM),
        scratch_shapes=[pltpu.SemaphoreType.DMA, pltpu.SemaphoreType.DMA((N_DEV,)), pltpu.SemaphoreType.DMA((N_DEV,))],
        compiler_params=pltpu.CompilerParams(collective_id=0, has_side_effects=True),
        name="gather_tokens",
    )(tok_block)


def head_kernel(groups, vocab, hn_hbm, lab_hbm, norm_ref, table_ref, table_t_ref, dhn_ref, dtable_ref, lse_ref, pick_ref,
                hn_all, lab_all, lse_mine, lse_all, part_own, part_out, part_in, sum_in, dhn_acc,
                local_sems, ag_send, ag_recv, fw_send, lab_send, lab_recv, st_send, st_recv, d2_send, d2_recv, rs_send, rs_recv):
    me = lax.axis_index("fsdp")
    chunks = vocab // V_CHUNK
    pair_rows = 2 * UNIT

    lab_copy = pltpu.make_async_copy(lab_hbm, lab_all.at[0], local_sems.at[0])
    lab_copy.start()
    hn_copy = pltpu.make_async_copy(hn_hbm, hn_all.at[:, 0], local_sems.at[1])
    hn_copy.start()
    meet_all(me)
    lab_copy.wait()

    def label_send(step):
        return remote(lab_all.at[0], lab_all.at[step], lab_send.at[step], lab_recv.at[step], peer_of(me, step))

    def own_send(step, group):
        return remote(hn_all.at[group, 0], hn_all.at[group, step], ag_send.at[step, group], ag_recv.at[step, group], peer_of(me, step))

    def forward(step, group):
        return remote(hn_all.at[group, step], hn_all.at[group, step + 1], fw_send.at[step, group], ag_recv.at[step + 1, group], peer_of(me, 1))

    def stat_send(step, group):
        return remote(lse_mine.at[group], lse_all.at[group, step], st_send.at[step, group], st_recv.at[step, group], peer_of(me, step))

    def part_send(group, pair):
        return remote(part_out.at[group, pair], part_in.at[group, pair], d2_send.at[group, pair], d2_recv.at[group, pair], peer_of(me, 1))

    def home_send(group, pair):
        return remote(part_own.at[group, pair], sum_in.at[group, pair], rs_send.at[group, pair], rs_recv.at[group, pair], peer_of(me, 2 * pair))

    hn_copy.wait()

    @pl.loop(0, groups)
    def _(group):
        for step in (1, 2, 4, 6):
            own_send(step, group).start()

    for step in range(1, N_DEV):
        label_send(step).start()
    dtable_ref[...] = jnp.zeros_like(dtable_ref)
    pick_ref[...] = jnp.zeros_like(pick_ref)

    def table_rows(chunk):
        return table_ref[pl.ds(pl.multiple_of(chunk * V_CHUNK, V_CHUNK), V_CHUNK), :]

    @pl.loop(0, groups)
    def _(group):
        @pl.loop(0, 4)
        def _(pair):
            @pl.when(pair > 0)
            def _():
                own_send(2 * pair, group).wait_recv()
                forward(2 * pair, group).start()

            @pl.when(pair == 0)
            def _():
                own_send(1, group).wait_recv()

            @pl.when(pair > 0)
            def _():
                forward(2 * pair, group).wait_recv()

            tile = hn_all[group, pl.ds(2 * pair, 2)].reshape(pair_rows, 256)
            run_max = jnp.full((8, pair_rows), -jnp.inf, jnp.float32)
            run_sum = jnp.zeros((8, pair_rows), jnp.float32)
            for chunk in range(chunks):
                logits = lax.dot_general(table_rows(chunk), tile, ROW_CONTRACT, preferred_element_type=jnp.float32)
                logits = logits.reshape(V_CHUNK // 8, 8, pair_rows)
                new_max = jnp.maximum(run_max, jnp.max(logits, axis=0))
                new_scaled = new_max * LOG2E
                run_sum = run_sum * jnp.exp2(run_max * LOG2E - new_scaled) + jnp.sum(jnp.exp2(logits * LOG2E - new_scaled[None]), axis=0)
                run_max = new_max
            scaled = run_max * LOG2E
            top = jnp.max(scaled, axis=0, keepdims=True)
            total = jnp.sum(run_sum * jnp.exp2(scaled - top), axis=0, keepdims=True)
            lse_mine[group, pair] = top + jnp.log2(total)

        @pl.when(group > 0)
        def _():
            for step in range(1, N_DEV):
                stat_send(step, group - 1).start()

    for step in range(1, N_DEV):
        label_send(step).wait_recv()

    log2_n = norm_ref[0:1, :]
    log2_n = jnp.concatenate([log2_n] * (pair_rows // 128), axis=1)
    inv_n = norm_ref[1:2, :]
    inv_n = jnp.concatenate([inv_n] * (pair_rows // 128), axis=1)
    row_iota = lax.broadcasted_iota(jnp.int32, (V_CHUNK, pair_rows), 0)

    def finish_pair(group, pair):
        part_send(group, pair).wait_recv()
        part_own[group, pair] = part_own[group, pair] + part_in[group, pair]

    @pl.loop(0, groups)
    def _(group):
        @pl.when(group == 0)
        def _():
            for step in range(1, N_DEV):
                stat_send(step, groups - 1).start()

        for step in range(1, N_DEV):
            stat_send(step, group).wait_recv()

        @pl.loop(0, 4)
        def _(turn):
            pair = 3 - turn
            low, high = [], []
            for step in range(N_DEV):
                source = lse_mine.at[group] if step == 0 else lse_all.at[group, step]
                row = source[pair_xor(pair, step // 2)]
                halves = [row[:, :UNIT], row[:, UNIT:]]
                low.append(halves[step % 2])
                high.append(halves[1 - step % 2])
            both = [jnp.concatenate(two, axis=1) for two in zip(low, high)]
            top = functools.reduce(jnp.maximum, both)
            lse = top + jnp.log2(sum(jnp.exp2(part - top) for part in both))
            label = jnp.concatenate([lab_all[2 * pair, group], lab_all[2 * pair + 1, group]], axis=1)
            valid = label >= 0
            shift = jnp.where(valid, lse + log2_n, 1e30)

            @pl.when(pair == 0)
            def _():
                lse_ref[group] = jnp.where(valid, lse, 0.0)[:, :UNIT]

            tile = hn_all[group, pl.ds(2 * pair, 2)].reshape(pair_rows, 256)
            local_label = label - me * vocab
            picked = jnp.zeros((8, pair_rows), jnp.float32)
            for chunk in range(chunks):
                logits = lax.dot_general(table_rows(chunk), tile, ROW_CONTRACT, preferred_element_type=jnp.float32)
                is_label = row_iota == (local_label - chunk * V_CHUNK)
                picked += jnp.sum(jnp.where(is_label, logits, 0.0).reshape(V_CHUNK // 8, 8, pair_rows), axis=0)
                prob = jnp.exp2(logits * LOG2E - shift)
                d_logits = jnp.where(is_label, prob - inv_n, prob).astype(jnp.bfloat16)
                rows = pl.ds(chunk * V_CHUNK, V_CHUNK)
                dtable_ref[rows, :] += jnp.dot(d_logits, tile, preferred_element_type=jnp.float32)
                d_part = jnp.dot(table_t_ref[:, rows], d_logits, preferred_element_type=jnp.float32)
                if chunk == 0:
                    dhn_acc[...] = d_part
                else:
                    dhn_acc[...] += d_part
            pick_ref[...] += picked
            part_own[group, pair] = dhn_acc[:, :UNIT]
            part_out[group, pair] = dhn_acc[:, UNIT:]
            part_send(group, pair).start()

            @pl.when(turn > 0)
            def _():
                finish_pair(group, pair + 1)
                home_send(group, pair + 1).start()

            @pl.when((turn == 0) & (group > 0))
            def _():
                finish_pair(group - 1, 0)

    finish_pair(groups - 1, 0)

    @pl.loop(0, groups)
    def _(group):
        total = part_own[group, 0]
        for pair in (1, 2, 3):
            home_send(group, pair).wait_recv()
            total = total + sum_in[group, pair]
        dhn_ref[group] = total.T
        for step in (1, 2, 4, 6):
            own_send(step, group).wait_send()
        for step in (2, 4, 6):
            forward(step, group).wait_send()
        for step in range(1, N_DEV):
            stat_send(step, group).wait_send()
        for pair in range(4):
            part_send(group, pair).wait_send()
        for pair in (1, 2, 3):
            home_send(group, pair).wait_send()

    for step in range(1, N_DEV):
        label_send(step).wait_send()


def head_call(h_norm, labels, norm_rows, table, table_t, groups):
    vocab = table.shape[0]
    dma = pltpu.SemaphoreType.DMA
    vmem = pl.BlockSpec(memory_space=pltpu.VMEM)
    hbm = pl.BlockSpec(memory_space=pl.ANY)
    f32, bf16 = jnp.float32, jnp.bfloat16
    tokens = N_DEV * groups * UNIT
    return pl.pallas_call(
        functools.partial(head_kernel, groups, vocab),
        out_shape=(
            jax.ShapeDtypeStruct((groups, UNIT, 256), f32),
            jax.ShapeDtypeStruct((vocab, 256), f32),
            jax.ShapeDtypeStruct((groups, 1, UNIT), f32),
            jax.ShapeDtypeStruct((8, 2 * UNIT), f32),
        ),
        in_specs=[hbm, hbm, vmem, vmem, vmem],
        out_specs=(vmem, vmem, vmem, vmem),
        scratch_shapes=[
            pltpu.VMEM((groups, N_DEV, UNIT, 256), bf16),
            pltpu.VMEM((N_DEV, groups, 1, UNIT), jnp.int32),
            pltpu.VMEM((groups, 4, 1, 2 * UNIT), f32),
            pltpu.VMEM((groups, N_DEV, 4, 1, 2 * UNIT), f32),
            pltpu.VMEM((groups, 4, 256, UNIT), f32),
            pltpu.VMEM((groups, 4, 256, UNIT), f32),
            pltpu.VMEM((groups, 4, 256, UNIT), f32),
            pltpu.VMEM((groups, 4, 256, UNIT), f32),
            pltpu.VMEM((256, 2 * UNIT), f32),
            dma((2,)),
            dma((N_DEV, groups)),
            dma((N_DEV, groups)),
            dma((N_DEV, groups)),
            dma((N_DEV,)),
            dma((N_DEV,)),
            dma((N_DEV, groups)),
            dma((N_DEV, groups)),
            dma((groups, 4)),
            dma((groups, 4)),
            dma((groups, 4)),
            dma((groups, 4)),
        ],
        compiler_params=pltpu.CompilerParams(collective_id=1, has_side_effects=True, vmem_limit_bytes=VMEM_MAX),
        cost_estimate=pl.CostEstimate(flops=8 * tokens * vocab * 256, bytes_accessed=16 * vocab * 256, transcendentals=2 * tokens * vocab),
        name="head",
    )(h_norm, labels, norm_rows, table, table_t)


def rms_scale(rows_wide, norm_gain):
    inv_rms = lax.rsqrt(jnp.mean(rows_wide * rows_wide, axis=-1, keepdims=True) + NORM_EPS)
    return (rows_wide * inv_rms * norm_gain).astype(jnp.bfloat16), inv_rms


def mlp_forward(emb_rows, gain_mlp, gain_head, w_gate, w_up, w_down):
    emb_wide = emb_rows.astype(jnp.float32)
    a_norm, _ = rms_scale(emb_wide, gain_mlp)
    gate = jnp.dot(a_norm, w_gate, preferred_element_type=jnp.float32).astype(jnp.bfloat16)
    up = jnp.dot(a_norm, w_up, preferred_element_type=jnp.float32).astype(jnp.bfloat16)
    gate_wide = gate.astype(jnp.float32)
    act = (gate_wide * jax.nn.sigmoid(gate_wide) * up.astype(jnp.float32)).astype(jnp.bfloat16)
    hid = (emb_wide + jnp.dot(act, w_down, preferred_element_type=jnp.float32)).astype(jnp.bfloat16)
    h_norm, _ = rms_scale(hid.astype(jnp.float32), gain_head)
    return (hid, gate, up, act), h_norm


def back_kernel(groups, dhn_ref, x_hbm, hid_hbm, gate_hbm, up_hbm, act_hbm, gain1_ref, gain2_ref, w_gate_hbm, w_up_hbm, w_down_hbm, rows_ref, head_hbm, loss_ref,
                loss_out, dtable_ref, dgate_ref, dup_ref, ddown_ref,
                x_buf, hid_buf, gate_buf, up_buf, act_buf, w_gate, w_up, w_down, head_buf, dh_wide, dh_narrow, dh_t, a_t, da_acc, dp_buf, dq_buf, dx_parts, inv_buf,
                down_acc, down_core, down_first, down_second, wide_acc, wide_core, wide_first, wide_second, loss_all,
                in_sems, tile_sems, loss_send, loss_recv, core_send, core_recv, first_send, first_recv, second_send, second_recv):
    me = lax.axis_index("fsdp")
    core = me % 2
    first_step = 2 + 2 * core
    second_step = 4 - 2 * core
    chunk_w = 512
    chunks = w_gate.shape[1] // chunk_w
    f32, bf16 = jnp.float32, jnp.bfloat16

    whole = [(x_hbm, x_buf), (hid_hbm, hid_buf), (act_hbm, act_buf), (w_down_hbm, w_down), (w_gate_hbm, w_gate), (w_up_hbm, w_up), (head_hbm, head_buf)]
    loads = [pltpu.make_async_copy(src, dst, in_sems.at[i]) for i, (src, dst) in enumerate(whole)]
    tiles = [pltpu.make_async_copy(src, dst, tile_sems.at[i]) for i, (src, dst) in enumerate([(gate_hbm, gate_buf), (up_hbm, up_buf)])]
    for load in loads[:4] + tiles + loads[4:]:
        load.start()
    meet_all(me)

    def loss_copy(step):
        return remote(loss_ref, loss_all.at[step], loss_send.at[step], loss_recv.at[step], peer_of(me, step))

    for step in range(1, N_DEV):
        loss_copy(step).start()

    def piece(unit, step):
        if isinstance(unit, int) and unit == 0:
            return down_acc.at[peer_of(me, step)]
        return wide_acc.at[unit - 1, peer_of(me, step)]

    def core_copy(unit, pair):
        target = down_core.at[pair] if unit == 0 else wide_core.at[unit - 1, pair]
        return remote(piece(unit, 2 * pair + 1), target, core_send.at[unit, pair], core_recv.at[unit, pair], peer_of(me, 1))

    def first_copy(unit, which):
        target = down_first.at[which] if unit == 0 else wide_first.at[unit - 1, which]
        return remote(piece(unit, first_step if which == 0 else 6), target, first_send.at[unit, which], first_recv.at[unit, which], peer_of(me, first_step))

    def second_copy(unit):
        target = down_second if unit == 0 else wide_second.at[unit - 1]
        return remote(piece(unit, second_step), target, second_send.at[unit], second_recv.at[unit], peer_of(me, second_step))

    def send_core(unit):
        for pair in (1, 2, 3, 0):
            core_copy(unit, pair).start()

    def add_core(unit):
        for pair in (3, 2, 1, 0):
            core_copy(unit, pair).wait_recv()
            dst = piece(unit, 2 * pair)
            dst[...] = dst[...] + (down_core[pair] if unit == 0 else wide_core[unit - 1, pair])
        first_copy(unit, 1).start()
        first_copy(unit, 0).start()

    def add_first(unit):
        for which in (1, 0):
            first_copy(unit, which).wait_recv()
            dst = piece(unit, second_step if which == 1 else 0)
            dst[...] = dst[...] + (down_first[which] if unit == 0 else wide_first[unit - 1, which])
        second_copy(unit).start()

    def add_second(unit):
        second_copy(unit).wait_recv()
        if unit == 0:
            ddown_ref[...] = down_acc[me] + down_second[...]
        else:
            both = wide_acc[unit - 1, me] + wide_second[unit - 1]
            cols = slice((unit - 1) * chunk_w, unit * chunk_w)
            dgate_ref[:, cols] = both[0]
            dup_ref[:, cols] = both[1]

    loads[0].wait()
    loads[1].wait()

    @pl.loop(0, groups)
    def _(group):
        rows = pl.ds(pl.multiple_of(group * UNIT, UNIT), UNIT)
        hid = hid_buf[rows, :].astype(f32)
        inv_second = lax.rsqrt(jnp.mean(hid * hid, axis=-1, keepdims=True) + NORM_EPS)
        scaled = dhn_ref[group] * gain2_ref[...]
        d_hid = inv_second * (scaled - hid * (inv_second * inv_second) * jnp.mean(scaled * hid, axis=-1, keepdims=True))
        dh_wide[rows, :] = d_hid
        dh_narrow[rows, :] = d_hid.astype(bf16)
        dh_t[:, rows] = d_hid.astype(bf16).astype(f32).T.astype(bf16)
        emb = x_buf[rows, :].astype(f32)
        inv_first = lax.rsqrt(jnp.mean(emb * emb, axis=-1, keepdims=True) + NORM_EPS)
        a_norm = (emb * inv_first * gain1_ref[...]).astype(bf16)
        a_t[:, rows] = a_norm.astype(f32).T.astype(bf16)
        da_acc[rows, :] = jnp.zeros((UNIT, 256), f32)

    loads[2].wait()

    @pl.loop(0, N_DEV)
    def _(dev):
        cols = pl.ds(pl.multiple_of(dev * 256, 256), 256)
        down_acc[dev] = jnp.dot(dh_t[...], act_buf[:, cols], preferred_element_type=f32).T

    send_core(0)
    loads[3].wait()
    for tile in tiles:
        tile.wait()
    loads[4].wait()
    loads[5].wait()
    for chunk in range(chunks):
        cols = slice(chunk * chunk_w, (chunk + 1) * chunk_w)

        @pl.loop(0, groups)
        def _(group):
            rows = pl.ds(pl.multiple_of(group * UNIT, UNIT), UNIT)
            d_act = lax.dot_general(dh_narrow[rows, :], w_down[cols, :], ROW_CONTRACT, preferred_element_type=f32)
            gate = gate_buf[rows, cols].astype(f32)
            up = up_buf[rows, cols].astype(f32)
            sig = jax.nn.sigmoid(gate)
            d_up = (d_act * gate * sig).astype(bf16)
            d_gate = (d_act * up * sig * (1.0 + gate * (1.0 - sig))).astype(bf16)
            dp_buf[rows, :] = d_gate
            dq_buf[rows, :] = d_up
            da_acc[rows, :] += lax.dot_general(d_gate, w_gate[:, cols], ROW_CONTRACT, preferred_element_type=f32) + lax.dot_general(d_up, w_up[:, cols], ROW_CONTRACT, preferred_element_type=f32)

        grad_gate = jnp.dot(a_t[...], dp_buf[...], preferred_element_type=f32)
        wide_acc[chunk, :, 0] = grad_gate.reshape(N_DEV, 32, chunk_w)
        grad_up = jnp.dot(a_t[...], dq_buf[...], preferred_element_type=f32)
        wide_acc[chunk, :, 1] = grad_up.reshape(N_DEV, 32, chunk_w)
        send_core(chunk + 1)
        add_core(chunk)
        if chunk >= 1:
            add_first(chunk - 1)

    @pl.loop(0, groups)
    def _(group):
        rows = pl.ds(pl.multiple_of(group * UNIT, UNIT), UNIT)
        emb = x_buf[rows, :].astype(f32)
        inv_first = lax.rsqrt(jnp.mean(emb * emb, axis=-1, keepdims=True) + NORM_EPS)
        scaled = da_acc[rows, :] * gain1_ref[...]
        dx = dh_wide[rows, :] + inv_first * (scaled - emb * (inv_first * inv_first) * jnp.mean(scaled * emb, axis=-1, keepdims=True))
        high = dx.astype(bf16)
        rest = dx - high.astype(f32)
        middle = rest.astype(bf16)
        dx_parts[rows, 0:256] = high
        dx_parts[rows, 256:512] = middle
        dx_parts[rows, 512:768] = (rest - middle.astype(f32)).astype(bf16)

    add_core(chunks)
    add_first(chunks - 1)
    loads[6].wait()
    row_block = 512
    blocks = head_buf.shape[0] // row_block
    row_iota = lax.broadcasted_iota(jnp.int32, (row_block, UNIT), 0)

    def scatter_block(block):
        base = block * row_block
        rows = pl.ds(pl.multiple_of(base, row_block), row_block)
        picks = jnp.concatenate([jnp.where(row_iota == rows_ref[group] - base, 1.0, 0.0).astype(bf16) for group in range(groups)], axis=1)
        parts = jnp.dot(picks, dx_parts[...], preferred_element_type=f32)
        dtable_ref[rows, :] = head_buf[rows, :] + (parts[:, 0:256] + (parts[:, 256:512] + parts[:, 512:768]))

    @pl.loop(0, blocks // 2)
    def _(block):
        scatter_block(block)

    add_first(chunks)

    @pl.loop(blocks // 2, blocks)
    def _(block):
        scatter_block(block)

    total = loss_ref[...]
    for step in range(1, N_DEV):
        loss_copy(step).wait_recv()
        total = total + loss_all[step]
    loss_out[...] = total
    for unit in range(chunks + 1):
        add_second(unit)
    for step in range(1, N_DEV):
        loss_copy(step).wait_send()
    for unit in range(chunks + 1):
        for pair in range(4):
            core_copy(unit, pair).wait_send()
        first_copy(unit, 0).wait_send()
        first_copy(unit, 1).wait_send()
        second_copy(unit).wait_send()


def back_call(d_hnorm, x_rows, hid, gate, up, act, gain_mlp, gain_head, w_gate, w_up, w_down, row_id, head_grad, loss_part):
    groups, _, width = d_hnorm.shape
    slots, wide = gate.shape
    vocab = head_grad.shape[0]
    chunks = wide // 512
    units = chunks + 1
    f32, bf16 = jnp.float32, jnp.bfloat16
    dma = pltpu.SemaphoreType.DMA
    vmem = pl.BlockSpec(memory_space=pltpu.VMEM)
    hbm = pl.BlockSpec(memory_space=pl.ANY)
    piece_d = (wide // N_DEV, width)
    piece_w = (2, width // N_DEV, 512)
    return pl.pallas_call(
        functools.partial(back_kernel, groups),
        out_shape=(
            jax.ShapeDtypeStruct((8, 128), f32),
            jax.ShapeDtypeStruct((vocab, width), f32),
            jax.ShapeDtypeStruct((width // N_DEV, wide), f32),
            jax.ShapeDtypeStruct((width // N_DEV, wide), f32),
            jax.ShapeDtypeStruct(piece_d, f32),
        ),
        in_specs=[vmem, hbm, hbm, hbm, hbm, hbm, vmem, vmem, hbm, hbm, hbm, vmem, hbm, vmem],
        out_specs=(vmem,) * 5,
        scratch_shapes=[
            pltpu.VMEM((slots, width), bf16),
            pltpu.VMEM((slots, width), bf16),
            pltpu.VMEM((slots, wide), bf16),
            pltpu.VMEM((slots, wide), bf16),
            pltpu.VMEM((slots, wide), bf16),
            pltpu.VMEM((width, wide), bf16),
            pltpu.VMEM((width, wide), bf16),
            pltpu.VMEM((wide, width), bf16),
            pltpu.VMEM((vocab, width), f32),
            pltpu.VMEM((slots, width), f32),
            pltpu.VMEM((slots, width), bf16),
            pltpu.VMEM((width, slots), bf16),
            pltpu.VMEM((width, slots), bf16),
            pltpu.VMEM((slots, width), f32),
            pltpu.VMEM((slots, 512), bf16),
            pltpu.VMEM((slots, 512), bf16),
            pltpu.VMEM((slots, 3 * width), bf16),
            pltpu.VMEM((8, 128), f32),
            pltpu.VMEM((N_DEV,) + piece_d, f32),
            pltpu.VMEM((4,) + piece_d, f32),
            pltpu.VMEM((2,) + piece_d, f32),
            pltpu.VMEM(piece_d, f32),
            pltpu.VMEM((chunks, N_DEV) + piece_w, f32),
            pltpu.VMEM((chunks, 4) + piece_w, f32),
            pltpu.VMEM((chunks, 2) + piece_w, f32),
            pltpu.VMEM((chunks,) + piece_w, f32),
            pltpu.VMEM((N_DEV, 8, 128), f32),
            dma((7,)),
            dma((2,)),
            dma((N_DEV,)),
            dma((N_DEV,)),
            dma((units, 4)),
            dma((units, 4)),
            dma((units, 2)),
            dma((units, 2)),
            dma((units,)),
            dma((units,)),
        ],
        compiler_params=pltpu.CompilerParams(collective_id=2, has_side_effects=True, vmem_limit_bytes=VMEM_MAX),
        cost_estimate=pl.CostEstimate(flops=16 * slots * wide * width, bytes_accessed=6 * slots * wide, transcendentals=slots * wide),
        name="back",
    )(d_hnorm, x_rows, hid, gate, up, act, gain_mlp.reshape(1, width), gain_head.reshape(1, width), w_gate, w_up, w_down, row_id, head_grad, loss_part)


GROUPS = 7


def solution(mesh):
    def gather_rows(row_shard):
        return lax.all_gather(row_shard, "fsdp", axis=0, tiled=True)

    def device_step(tok_ids, tok_labels, loss_mask, table_shard, gain_mlp, gain_head, gate_shard, up_shard, down_shard):
        me = lax.axis_index("fsdp")
        vocab, width = table_shard.shape
        vocab_all = vocab * N_DEV
        slots = GROUPS * UNIT
        gate_full, up_full, down_full = gather_rows(gate_shard), gather_rows(up_shard), gather_rows(down_shard)
        block = jnp.stack([tok_ids.reshape(-1, 128), tok_labels.reshape(-1, 128), loss_mask.reshape(-1, 128)])
        every = gather_tokens(block)
        ids, labels, mask = every[:, 0].reshape(-1), every[:, 1].reshape(-1), every[:, 2].reshape(-1)
        count = jnp.sum(mask).astype(jnp.float32)
        owner = ids // vocab
        loads = [jnp.sum(jnp.where(owner == dev, mask, 0)) for dev in range(N_DEV)]
        rounds = (functools.reduce(jnp.maximum, loads) + slots - 1) // slots
        last = jnp.int32(2**31 - 1)
        packed = jnp.where((owner == me) & (mask != 0), (ids - me * vocab) * vocab_all + labels, last)
        packed = jnp.sort(packed)
        most = -(-ids.shape[0] // slots) * slots
        packed = jnp.concatenate([packed, jnp.full((most - ids.shape[0],), last)])
        norm_rows = jnp.zeros((8, 128), jnp.float32).at[0].set(jnp.log2(count)).at[1].set(1.0 / count)
        table_t = table_shard.T

        def one_round(turn):
            mine = lax.dynamic_slice(packed, (turn * slots,), (slots,))
            valid = mine != last
            row_id = jnp.where(valid, mine // vocab_all, 0)
            label = jnp.where(valid, mine % vocab_all, -1)
            x_rows = jnp.take(table_shard, row_id, axis=0)
            (hid, gate, up, act), h_norm = mlp_forward(x_rows, gain_mlp, gain_head, gate_full, up_full, down_full)
            d_hnorm, head_grad, lse, picked = head_call(h_norm.reshape(GROUPS, UNIT, width), label.reshape(GROUPS, 1, UNIT), norm_rows, table_shard, table_t, GROUPS)
            part = (jnp.sum(lse) * LN2 - jnp.sum(picked)) / count
            loss_part = jnp.broadcast_to(part, (8, 128))
            return back_call(d_hnorm, x_rows, hid, gate, up, act, gain_mlp, gain_head, gate_full, up_full, down_full, row_id.reshape(GROUPS, 1, UNIT), head_grad, loss_part)

        def more_rounds(sums):
            def step(state):
                extra = one_round(state[0])
                return (state[0] + 1, tuple(old + new for old, new in zip(state[1], extra)))

            return lax.while_loop(lambda state: state[0] < rounds, step, (jnp.int32(1), tuple(sums)))[1]

        sums = lax.cond(rounds > 1, more_rounds, tuple, one_round(jnp.int32(0)))
        loss, g_table, g_gate, g_up, g_down = sums
        return (loss[0, 0], g_table, g_gate, g_up, g_down)

    row_spec = P("fsdp", None)
    tok_spec = P("fsdp")
    return jax.shard_map(device_step, mesh=mesh, in_specs=(tok_spec, tok_spec, tok_spec, row_spec, P(), P(), row_spec, row_spec, row_spec), out_specs=(P(), row_spec, row_spec, row_spec, row_spec), check_vma=False)
```

```python
import functools
import math

import jax
import jax.numpy as jnp
from jax import lax
from jax.experimental import pallas as pl
from jax.experimental.pallas import tpu as pltpu
from jax.sharding import PartitionSpec as P

NORM_EPS = 1e-6
ROW_CONTRACT = (((1,), (1,)), ((), ()))
TOK_CONTRACT = (((0,), (0,)), ((), ()))
MESH = pl.DeviceIdType.MESH
LOG2E = math.log2(math.e)
LN2 = math.log(2.0)
N_DEV = 8
UNIT = 256
V_CHUNK = 1024
VMEM_MAX = 67_043_328
LAST_KEY = 2**31 - 1
WIDE_CHUNK = 1024


def peer_of(me, step):
    core = (me % 2 + step % 2) % 2
    col = ((me // 2) % 2 + (step // 2) % 2) % 2
    row = (me // 4 + step // 4) % 2
    return row * 4 + col * 2 + core


def pair_xor(pair, other):
    return ((pair // 2 + other // 2) % 2) * 2 + (pair % 2 + other % 2) % 2


def meet_all(me):
    barrier = pltpu.get_barrier_semaphore()
    for step in range(1, N_DEV):
        pl.semaphore_signal(barrier, inc=1, device_id=(peer_of(me, step),), device_id_type=MESH)
    pl.semaphore_wait(barrier, N_DEV - 1)


def remote(src, dst, send_sem, recv_sem, target):
    return pltpu.make_async_remote_copy(src_ref=src, dst_ref=dst, send_sem=send_sem, recv_sem=recv_sem, device_id=(target,), device_id_type=MESH)


def tokens_kernel(ids_hbm, labels_hbm, mask_hbm, table_hbm, packed_ref, info_ref, table_t_ref, every, table_buf, local_sems, send_sems, recv_sems):
    me = lax.axis_index("fsdp")
    vocab = table_buf.shape[0]
    own = [pltpu.make_async_copy(src, every.at[which, 0], local_sems.at[which]) for which, src in enumerate((ids_hbm, labels_hbm, mask_hbm))]
    table_copy = pltpu.make_async_copy(table_hbm, table_buf, local_sems.at[3])
    for copy in own + [table_copy]:
        copy.start()
    meet_all(me)
    for copy in own:
        copy.wait()
    copies = []
    for step in range(1, N_DEV):
        copy = remote(every.at[:, 0], every.at[:, step], send_sems.at[step], recv_sems.at[step], peer_of(me, step))
        copy.start()
        copies.append(copy)
    table_copy.wait()

    @pl.loop(0, vocab // 512)
    def _(block):
        rows = pl.ds(pl.multiple_of(block * 512, 512), 512)
        table_t_ref[:, rows] = table_buf[rows, :].astype(jnp.float32).T.astype(jnp.bfloat16)

    for copy in copies:
        copy.wait()
    ids, labels, mask = every[0], every[1], every[2]
    local = ids - me * vocab
    mine = (local >= 0) & (local < vocab) & (mask != 0)
    packed_ref[...] = jnp.where(mine, local * (vocab * N_DEV) + labels, LAST_KEY)
    weight = mask.astype(jnp.float32)

    def total(rows):
        return jnp.sum(jnp.sum(jnp.sum(rows, axis=0), axis=0, keepdims=True), axis=1, keepdims=True)

    count = total(weight)
    load = jnp.zeros((1, 1), jnp.float32)
    for dev in range(N_DEV):
        here = (ids >= dev * vocab) & (ids < (dev + 1) * vocab)
        load = jnp.maximum(load, total(jnp.where(here, weight, 0.0)))
    info_ref[0:1, :] = jnp.broadcast_to(jnp.log2(count), (1, 128))
    info_ref[1:2, :] = jnp.broadcast_to(1.0 / count, (1, 128))
    info_ref[2:3, :] = jnp.broadcast_to(load, (1, 128))
    info_ref[3:8, :] = jnp.zeros((5, 128), jnp.float32)


def gather_tokens(ids, labels, mask, table):
    rows = (ids.shape[0] // 128, 128)
    vocab, width = table.shape
    dma = pltpu.SemaphoreType.DMA
    vmem = pl.BlockSpec(memory_space=pltpu.VMEM)
    hbm = pl.BlockSpec(memory_space=pl.ANY)
    return pl.pallas_call(
        tokens_kernel,
        out_shape=(
            jax.ShapeDtypeStruct((N_DEV,) + rows, jnp.int32),
            jax.ShapeDtypeStruct((8, 128), jnp.float32),
            jax.ShapeDtypeStruct((width, vocab), jnp.bfloat16),
        ),
        in_specs=[hbm] * 4,
        out_specs=(vmem,) * 3,
        scratch_shapes=[pltpu.VMEM((3, N_DEV) + rows, jnp.int32), pltpu.VMEM((vocab, width), jnp.bfloat16), dma((4,)), dma((N_DEV,)), dma((N_DEV,))],
        compiler_params=pltpu.CompilerParams(collective_id=0, has_side_effects=True),
        name="gather_tokens",
    )(ids.reshape(rows), labels.reshape(rows), mask.reshape(rows), table)


def head_kernel(groups, vocab, hn_hbm, lab_hbm, norm_ref, table_ref, table_t_ref, dhn_ref, dtable_ref, lse_ref, pick_ref,
                hn_all, lab_all, lse_mine, lse_all, part_own, part_out, part_in, sum_in, dhn_acc,
                local_sems, ag_send, ag_recv, fw_send, lab_send, lab_recv, st_send, st_recv, d2_send, d2_recv, rs_send, rs_recv):
    me = lax.axis_index("fsdp")
    chunks = vocab // V_CHUNK
    pair_rows = 2 * UNIT

    lab_copy = pltpu.make_async_copy(lab_hbm, lab_all.at[0], local_sems.at[0])
    lab_copy.start()
    hn_copy = pltpu.make_async_copy(hn_hbm, hn_all.at[:, 0], local_sems.at[1])
    hn_copy.start()
    meet_all(me)
    lab_copy.wait()

    def label_send(step):
        return remote(lab_all.at[0], lab_all.at[step], lab_send.at[step], lab_recv.at[step], peer_of(me, step))

    def own_send(step, group):
        return remote(hn_all.at[group, 0], hn_all.at[group, step], ag_send.at[step, group], ag_recv.at[step, group], peer_of(me, step))

    def forward(step, group):
        return remote(hn_all.at[group, step], hn_all.at[group, step + 1], fw_send.at[step, group], ag_recv.at[step + 1, group], peer_of(me, 1))

    def stat_send(step, group):
        return remote(lse_mine.at[group], lse_all.at[group, step], st_send.at[step, group], st_recv.at[step, group], peer_of(me, step))

    def part_send(group, pair):
        return remote(part_out.at[group, pair], part_in.at[group, pair], d2_send.at[group, pair], d2_recv.at[group, pair], peer_of(me, 1))

    def home_send(group, pair):
        return remote(part_own.at[group, pair], sum_in.at[group, pair], rs_send.at[group, pair], rs_recv.at[group, pair], peer_of(me, 2 * pair))

    hn_copy.wait()

    @pl.loop(0, groups)
    def _(group):
        for step in (1, 2, 4, 6):
            own_send(step, group).start()

    for step in range(1, N_DEV):
        label_send(step).start()
    dtable_ref[...] = jnp.zeros_like(dtable_ref)
    pick_ref[...] = jnp.zeros_like(pick_ref)

    def table_rows(chunk):
        return table_ref[pl.ds(pl.multiple_of(chunk * V_CHUNK, V_CHUNK), V_CHUNK), :]

    @pl.loop(0, groups)
    def _(group):
        @pl.loop(0, 4)
        def _(pair):
            def pass_on(pair):
                own_send(2 * pair, group).wait_recv()
                forward(2 * pair, group).start()

            @pl.when((pair == 1) & (group == 0))
            def _():
                pass_on(1)

            @pl.when((pair < 3) & (pair + group > 0))
            def _():
                pass_on(pair + 1)

            @pl.when(pair == 0)
            def _():
                own_send(1, group).wait_recv()

            @pl.when(pair > 0)
            def _():
                forward(2 * pair, group).wait_recv()

            tile = hn_all[group, pl.ds(2 * pair, 2)].reshape(pair_rows, 256)
            run_max = jnp.full((8, pair_rows), -jnp.inf, jnp.float32)
            run_sum = jnp.zeros((8, pair_rows), jnp.float32)
            for chunk in range(chunks):
                logits = lax.dot_general(table_rows(chunk), tile, ROW_CONTRACT, preferred_element_type=jnp.float32)
                logits = logits.reshape(V_CHUNK // 8, 8, pair_rows)
                new_max = jnp.maximum(run_max, jnp.max(logits, axis=0))
                new_scaled = new_max * LOG2E
                run_sum = run_sum * jnp.exp2(run_max * LOG2E - new_scaled) + jnp.sum(jnp.exp2(logits * LOG2E - new_scaled[None]), axis=0)
                run_max = new_max
            scaled = run_max * LOG2E
            top = jnp.max(scaled, axis=0, keepdims=True)
            total = jnp.sum(run_sum * jnp.exp2(scaled - top), axis=0, keepdims=True)
            lse_mine[group, pair] = top + jnp.log2(total)

        @pl.when(group > 0)
        def _():
            for step in range(1, N_DEV):
                stat_send(step, group - 1).start()

    for step in range(1, N_DEV):
        label_send(step).wait_recv()

    log2_n = norm_ref[0:1, :]
    log2_n = jnp.concatenate([log2_n] * (pair_rows // 128), axis=1)
    inv_n = norm_ref[1:2, :]
    inv_n = jnp.concatenate([inv_n] * (pair_rows // 128), axis=1)
    row_iota = lax.broadcasted_iota(jnp.int32, (V_CHUNK, pair_rows), 0)

    def finish_pair(group, pair):
        part_send(group, pair).wait_recv()
        part_own[group, pair] = part_own[group, pair] + part_in[group, pair]

    @pl.loop(0, groups)
    def _(group):
        @pl.when(group == 0)
        def _():
            for step in range(1, N_DEV):
                stat_send(step, groups - 1).start()

        for step in range(1, N_DEV):
            stat_send(step, group).wait_recv()

        @pl.loop(0, 4)
        def _(turn):
            pair = 3 - turn
            low, high = [], []
            for step in range(N_DEV):
                source = lse_mine.at[group] if step == 0 else lse_all.at[group, step]
                row = source[pair_xor(pair, step // 2)]
                halves = [row[:, :UNIT], row[:, UNIT:]]
                low.append(halves[step % 2])
                high.append(halves[1 - step % 2])
            both = [jnp.concatenate(two, axis=1) for two in zip(low, high)]
            top = functools.reduce(jnp.maximum, both)
            lse = top + jnp.log2(sum(jnp.exp2(part - top) for part in both))
            label = jnp.concatenate([lab_all[2 * pair, group], lab_all[2 * pair + 1, group]], axis=1)
            valid = label >= 0
            shift = jnp.where(valid, lse + log2_n, 1e30)

            @pl.when(pair == 0)
            def _():
                lse_ref[group] = jnp.where(valid, lse, 0.0)[:, :UNIT]

            tile = hn_all[group, pl.ds(2 * pair, 2)].reshape(pair_rows, 256)
            local_label = label - me * vocab
            sub_row = lax.broadcasted_iota(jnp.int32, (8, pair_rows), 0)
            tile_row = jnp.where(local_label % 8 == sub_row, local_label // 8, -1)
            block_row = lax.broadcasted_iota(jnp.int32, (V_CHUNK // 8, 8, pair_rows), 0)
            picked = jnp.zeros((8, pair_rows), jnp.float32)
            for chunk in range(chunks):
                logits = lax.dot_general(table_rows(chunk), tile, ROW_CONTRACT, preferred_element_type=jnp.float32)
                logits = logits.reshape(V_CHUNK // 8, 8, pair_rows)
                is_label = block_row == (tile_row - chunk * (V_CHUNK // 8))[None]
                for row in range(V_CHUNK // 8):
                    picked = jnp.where(is_label[row], logits[row], picked)
                prob = jnp.exp2(logits * LOG2E - shift[None])
                d_logits = jnp.where(is_label, prob - inv_n[None], prob).reshape(V_CHUNK, pair_rows).astype(jnp.bfloat16)
                rows = pl.ds(chunk * V_CHUNK, V_CHUNK)
                dtable_ref[rows, :] += jnp.dot(d_logits, tile, preferred_element_type=jnp.float32)
                d_part = jnp.dot(table_t_ref[:, rows], d_logits, preferred_element_type=jnp.float32)
                if chunk == 0:
                    dhn_acc[...] = d_part
                else:
                    dhn_acc[...] += d_part
            pick_ref[...] += picked
            part_own[group, pair] = dhn_acc[:, :UNIT]
            part_out[group, pair] = dhn_acc[:, UNIT:]
            part_send(group, pair).start()

            @pl.when(turn > 0)
            def _():
                finish_pair(group, pair + 1)
                home_send(group, pair + 1).start()

            @pl.when((turn == 0) & (group > 0))
            def _():
                finish_pair(group - 1, 0)

    finish_pair(groups - 1, 0)

    @pl.loop(0, groups)
    def _(group):
        total = part_own[group, 0]
        for pair in (1, 2, 3):
            home_send(group, pair).wait_recv()
            total = total + sum_in[group, pair]
        dhn_ref[group] = total.T
        for step in (1, 2, 4, 6):
            own_send(step, group).wait_send()
        for step in (2, 4, 6):
            forward(step, group).wait_send()
        for step in range(1, N_DEV):
            stat_send(step, group).wait_send()
        for pair in range(4):
            part_send(group, pair).wait_send()
        for pair in (1, 2, 3):
            home_send(group, pair).wait_send()

    for step in range(1, N_DEV):
        label_send(step).wait_send()


def head_call(h_norm, labels, norm_rows, table, table_t, groups, variant=0):
    vocab = table.shape[0]
    dma = pltpu.SemaphoreType.DMA
    vmem = pl.BlockSpec(memory_space=pltpu.VMEM)
    hbm = pl.BlockSpec(memory_space=pl.ANY)
    f32, bf16 = jnp.float32, jnp.bfloat16
    tokens = N_DEV * groups * UNIT
    return pl.pallas_call(
        functools.partial(head_kernel, groups, vocab),
        out_shape=(
            jax.ShapeDtypeStruct((groups, UNIT, 256), f32),
            jax.ShapeDtypeStruct((vocab, 256), f32),
            jax.ShapeDtypeStruct((groups, 1, UNIT), f32),
            jax.ShapeDtypeStruct((8, 2 * UNIT), f32),
        ),
        in_specs=[hbm, hbm, vmem, vmem, vmem],
        out_specs=(vmem, vmem, vmem, vmem),
        scratch_shapes=[
            pltpu.VMEM((groups, N_DEV, UNIT, 256), bf16),
            pltpu.VMEM((N_DEV, groups, 1, UNIT), jnp.int32),
            pltpu.VMEM((groups, 4, 1, 2 * UNIT), f32),
            pltpu.VMEM((groups, N_DEV, 4, 1, 2 * UNIT), f32),
            pltpu.VMEM((groups, 4, 256, UNIT), f32),
            pltpu.VMEM((groups, 4, 256, UNIT), f32),
            pltpu.VMEM((groups, 4, 256, UNIT), f32),
            pltpu.VMEM((groups, 4, 256, UNIT), f32),
            pltpu.VMEM((256, 2 * UNIT), f32),
            dma((2,)),
            dma((N_DEV, groups)),
            dma((N_DEV, groups)),
            dma((N_DEV, groups)),
            dma((N_DEV,)),
            dma((N_DEV,)),
            dma((N_DEV, groups)),
            dma((N_DEV, groups)),
            dma((groups, 4)),
            dma((groups, 4)),
            dma((groups, 4)),
            dma((groups, 4)),
        ],
        compiler_params=pltpu.CompilerParams(collective_id=1 + 2 * variant, has_side_effects=True, vmem_limit_bytes=VMEM_MAX),
        cost_estimate=pl.CostEstimate(flops=8 * tokens * vocab * 256, bytes_accessed=16 * vocab * 256, transcendentals=2 * tokens * vocab),
        name="head",
    )(h_norm, labels, norm_rows, table, table_t)


def rms_scale(rows_wide, norm_gain):
    inv_rms = lax.rsqrt(jnp.mean(rows_wide * rows_wide, axis=-1, keepdims=True) + NORM_EPS)
    return (rows_wide * inv_rms * norm_gain).astype(jnp.bfloat16), inv_rms


def forward_kernel(*refs):
    wide_slots, down_slots = refs[:N_DEV], refs[N_DEV : 2 * N_DEV]
    x_ref, gain1_ref, gain2_ref, hid_ref, gate_ref, up_ref, act_ref, hn_ref, gate_hbm, up_hbm, down_hbm, w_gate, w_up, w_down, in_sems, out_sems = refs[2 * N_DEV :]
    f32, bf16 = jnp.float32, jnp.bfloat16
    me = lax.axis_index("fsdp")
    rows_w, rows_d = wide_slots[0].shape[1], down_slots[0].shape[0]
    outs = [pltpu.make_async_copy(src, dst, out_sems.at[i]) for i, (src, dst) in enumerate([(w_gate, gate_hbm), (w_up, up_hbm), (w_down, down_hbm)])]

    @pl.when(pl.program_id(0) == 0)
    def _():
        copies = []
        for step in range(N_DEV):
            dev = peer_of(me, step)
            copies.append(pltpu.make_async_copy(wide_slots[step].at[0], w_gate.at[pl.ds(dev * rows_w, rows_w)], in_sems.at[step, 0]))
            copies.append(pltpu.make_async_copy(wide_slots[step].at[1], w_up.at[pl.ds(dev * rows_w, rows_w)], in_sems.at[step, 1]))
            copies.append(pltpu.make_async_copy(down_slots[step], w_down.at[pl.ds(dev * rows_d, rows_d)], in_sems.at[step, 2]))
        for copy in copies:
            copy.start()
        for copy in copies:
            copy.wait()
        for copy in outs:
            copy.start()

    emb = x_ref[...].astype(f32)
    a_norm, _ = rms_scale(emb, gain1_ref[...])
    for chunk in range(w_gate.shape[1] // 512):
        cols = slice(chunk * 512, (chunk + 1) * 512)
        gate = jnp.dot(a_norm, w_gate[:, cols], preferred_element_type=f32).astype(bf16)
        up = jnp.dot(a_norm, w_up[:, cols], preferred_element_type=f32).astype(bf16)
        gate_ref[:, cols] = gate
        up_ref[:, cols] = up
        wide = gate.astype(f32)
        act_ref[:, cols] = (wide * jax.nn.sigmoid(wide) * up.astype(f32)).astype(bf16)
    hid = (emb + jnp.dot(act_ref[...], w_down[...], preferred_element_type=f32)).astype(bf16)
    hid_ref[...] = hid
    hn_ref[...], _ = rms_scale(hid.astype(f32), gain2_ref[...])

    @pl.when(pl.program_id(0) == pl.num_programs(0) - 1)
    def _():
        for copy in outs:
            copy.wait()


def forward_call(wide_slots, down_slots, x_rows, gain_mlp, gain_head, groups):
    slots, width = groups * UNIT, x_rows.shape[1]
    wide = wide_slots[0].shape[2]
    bf16 = jnp.bfloat16
    dma = pltpu.SemaphoreType.DMA
    hbm = pl.BlockSpec(memory_space=pl.ANY)
    gain = pl.BlockSpec((1, width), lambda i: (0, 0))
    narrow = pl.BlockSpec((UNIT, width), lambda i: (i, 0))
    broad = pl.BlockSpec((UNIT, wide), lambda i: (i, 0))
    full = [(width, wide), (width, wide), (wide, width)]
    return pl.pallas_call(
        forward_kernel,
        grid=(groups,),
        out_shape=[jax.ShapeDtypeStruct(shape, bf16) for shape in [(slots, width), (slots, wide), (slots, wide), (slots, wide), (slots, width)] + full],
        in_specs=[hbm] * (2 * N_DEV) + [narrow, gain, gain],
        out_specs=[narrow, broad, broad, broad, narrow, hbm, hbm, hbm],
        scratch_shapes=[pltpu.VMEM(shape, bf16) for shape in full] + [dma((N_DEV, 3)), dma((3,))],
        compiler_params=pltpu.CompilerParams(vmem_limit_bytes=VMEM_MAX),
        cost_estimate=pl.CostEstimate(flops=6 * slots * wide * width, bytes_accessed=6 * slots * wide, transcendentals=slots * wide),
        name="block_forward",
    )(*wide_slots, *down_slots, x_rows, gain_mlp.reshape(1, width), gain_head.reshape(1, width))


def back_kernel(groups, dhn_ref, x_hbm, hid_hbm, gate_hbm, up_hbm, act_hbm, gain1_ref, gain2_ref, w_gate_hbm, w_up_hbm, w_down_hbm, rows_ref, head_hbm, lse_ref, pick_ref, norm_ref,
                loss_out, dtable_ref, dgate_ref, dup_ref, ddown_ref,
                x_buf, hid_buf, gate_buf, up_buf, act_buf, w_gate, w_up, w_down, dh_wide, dh_narrow, dh_t, a_t, da_acc, dp_buf, dq_buf, dx_parts,
                down_acc, down_core, down_first, down_second, wide_acc, wide_core, wide_first, wide_second, loss_all, loss_ref,
                in_sems, tile_sems, loss_send, loss_recv, core_send, core_recv, first_send, first_recv, second_send, second_recv):
    me = lax.axis_index("fsdp")
    core = me % 2
    first_step = 2 + 2 * core
    second_step = 4 - 2 * core
    chunk_w = WIDE_CHUNK
    chunks = w_gate.shape[1] // chunk_w
    f32, bf16 = jnp.float32, jnp.bfloat16

    whole = [(x_hbm.at[pl.ds(0, groups * UNIT)], x_buf), (hid_hbm, hid_buf), (act_hbm, act_buf), (w_down_hbm, w_down), (w_gate_hbm, w_gate), (w_up_hbm, w_up), (head_hbm, dtable_ref)]
    loads = [pltpu.make_async_copy(src, dst, in_sems.at[i]) for i, (src, dst) in enumerate(whole)]
    tiles = [pltpu.make_async_copy(src, dst, tile_sems.at[i]) for i, (src, dst) in enumerate([(gate_hbm, gate_buf), (up_hbm, up_buf)])]
    for load in loads[:4] + tiles + loads[4:]:
        load.start()
    nats = jnp.sum(jnp.sum(lse_ref[...], axis=0), axis=1, keepdims=True) * LN2
    gold = jnp.sum(jnp.sum(pick_ref[...], axis=0, keepdims=True), axis=1, keepdims=True)
    loss_ref[...] = jnp.broadcast_to(nats - gold, (8, 128)) * norm_ref[1:2, :]
    meet_all(me)

    def loss_copy(step):
        return remote(loss_ref, loss_all.at[step], loss_send.at[step], loss_recv.at[step], peer_of(me, step))

    def piece(unit, step):
        if isinstance(unit, int) and unit == 0:
            return down_acc.at[peer_of(me, step)]
        return wide_acc.at[unit - 1, peer_of(me, step)]

    def core_copy(unit, pair):
        target = down_core.at[pair] if unit == 0 else wide_core.at[unit - 1, pair]
        return remote(piece(unit, 2 * pair + 1), target, core_send.at[unit, pair], core_recv.at[unit, pair], peer_of(me, 1))

    def first_copy(unit, which):
        target = down_first.at[which] if unit == 0 else wide_first.at[unit - 1, which]
        return remote(piece(unit, first_step if which == 0 else 6), target, first_send.at[unit, which], first_recv.at[unit, which], peer_of(me, first_step))

    def second_copy(unit):
        target = down_second if unit == 0 else wide_second.at[unit - 1]
        return remote(piece(unit, second_step), target, second_send.at[unit], second_recv.at[unit], peer_of(me, second_step))

    def send_core(unit):
        for pair in (1, 2, 3, 0):
            core_copy(unit, pair).start()

    def add_core(unit):
        for pair in (3, 2, 1, 0):
            core_copy(unit, pair).wait_recv()
            dst = piece(unit, 2 * pair)
            dst[...] = dst[...] + (down_core[pair] if unit == 0 else wide_core[unit - 1, pair])
        first_copy(unit, 1).start()
        first_copy(unit, 0).start()

    def add_first(unit):
        for which in (1, 0):
            first_copy(unit, which).wait_recv()
            dst = piece(unit, second_step if which == 1 else 0)
            dst[...] = dst[...] + (down_first[which] if unit == 0 else wide_first[unit - 1, which])
        second_copy(unit).start()

    def add_second(unit):
        second_copy(unit).wait_recv()
        if unit == 0:
            ddown_ref[...] = down_acc[me] + down_second[...]
        else:
            both = wide_acc[unit - 1, me] + wide_second[unit - 1]
            cols = slice((unit - 1) * chunk_w, unit * chunk_w)
            dgate_ref[:, cols] = both[0]
            dup_ref[:, cols] = both[1]

    loads[0].wait()
    loads[1].wait()

    @pl.loop(0, groups)
    def _(group):
        rows = pl.ds(pl.multiple_of(group * UNIT, UNIT), UNIT)
        hid = hid_buf[rows, :].astype(f32)
        inv_second = lax.rsqrt(jnp.mean(hid * hid, axis=-1, keepdims=True) + NORM_EPS)
        scaled = dhn_ref[group] * gain2_ref[...]
        d_hid = inv_second * (scaled - hid * (inv_second * inv_second) * jnp.mean(scaled * hid, axis=-1, keepdims=True))
        dh_wide[rows, :] = d_hid
        dh_narrow[rows, :] = d_hid.astype(bf16)
        dh_t[:, rows] = d_hid.astype(bf16).astype(f32).T.astype(bf16)
        emb = x_buf[rows, :].astype(f32)
        inv_first = lax.rsqrt(jnp.mean(emb * emb, axis=-1, keepdims=True) + NORM_EPS)
        a_norm = (emb * inv_first * gain1_ref[...]).astype(bf16)
        a_t[:, rows] = a_norm.astype(f32).T.astype(bf16)
        da_acc[rows, :] = jnp.zeros((UNIT, 256), f32)

    for step in range(1, N_DEV):
        loss_copy(step).start()
    loads[2].wait()

    @pl.loop(0, N_DEV)
    def _(dev):
        cols = pl.ds(pl.multiple_of(dev * 256, 256), 256)
        down_acc[dev] = jnp.dot(dh_t[...], act_buf[:, cols], preferred_element_type=f32).T

    send_core(0)
    loads[3].wait()
    for tile in tiles:
        tile.wait()
    loads[4].wait()
    loads[5].wait()
    for chunk in range(chunks):
        cols = slice(chunk * chunk_w, (chunk + 1) * chunk_w)

        @pl.loop(0, groups)
        def _(group):
            rows = pl.ds(pl.multiple_of(group * UNIT, UNIT), UNIT)
            d_act = lax.dot_general(dh_narrow[rows, :], w_down[cols, :], ROW_CONTRACT, preferred_element_type=f32)
            gate = gate_buf[rows, cols].astype(f32)
            up = up_buf[rows, cols].astype(f32)
            sig = jax.nn.sigmoid(gate)
            d_up = (d_act * gate * sig).astype(bf16)
            d_gate = (d_act * up * sig * (1.0 + gate * (1.0 - sig))).astype(bf16)
            dp_buf[rows, :] = d_gate
            dq_buf[rows, :] = d_up
            da_acc[rows, :] += lax.dot_general(d_gate, w_gate[:, cols], ROW_CONTRACT, preferred_element_type=f32) + lax.dot_general(d_up, w_up[:, cols], ROW_CONTRACT, preferred_element_type=f32)

        grad_gate = jnp.dot(a_t[...], dp_buf[...], preferred_element_type=f32)
        wide_acc[chunk, :, 0] = grad_gate.reshape(N_DEV, 32, chunk_w)
        grad_up = jnp.dot(a_t[...], dq_buf[...], preferred_element_type=f32)
        wide_acc[chunk, :, 1] = grad_up.reshape(N_DEV, 32, chunk_w)
        send_core(chunk + 1)
        add_core(chunk)
        if chunk >= 1:
            add_first(chunk - 1)

    @pl.loop(0, groups)
    def _(group):
        rows = pl.ds(pl.multiple_of(group * UNIT, UNIT), UNIT)
        emb = x_buf[rows, :].astype(f32)
        inv_first = lax.rsqrt(jnp.mean(emb * emb, axis=-1, keepdims=True) + NORM_EPS)
        scaled = da_acc[rows, :] * gain1_ref[...]
        dx = dh_wide[rows, :] + inv_first * (scaled - emb * (inv_first * inv_first) * jnp.mean(scaled * emb, axis=-1, keepdims=True))
        high = dx.astype(bf16)
        rest = dx - high.astype(f32)
        middle = rest.astype(bf16)
        dx_parts[rows, 0:256] = high
        dx_parts[rows, 256:512] = middle
        dx_parts[rows, 512:768] = (rest - middle.astype(f32)).astype(bf16)

    add_core(chunks)
    add_first(chunks - 1)
    loads[6].wait()
    row_block = 512
    blocks = dtable_ref.shape[0] // row_block
    row_iota = lax.broadcasted_iota(jnp.int32, (row_block, UNIT), 0)

    def scatter_block(block):
        base = block * row_block
        rows = pl.ds(pl.multiple_of(base, row_block), row_block)
        picks = jnp.concatenate([jnp.where(row_iota == rows_ref[group] - base, 1.0, 0.0).astype(bf16) for group in range(groups)], axis=1)
        parts = jnp.dot(picks, dx_parts[...], preferred_element_type=f32)
        dtable_ref[rows, :] += (parts[:, 0:256] + (parts[:, 256:512] + parts[:, 512:768]))

    @pl.loop(0, blocks // 2)
    def _(block):
        scatter_block(block)

    add_first(chunks)

    @pl.loop(blocks // 2, blocks)
    def _(block):
        scatter_block(block)

    total = loss_ref[...]
    for step in range(1, N_DEV):
        loss_copy(step).wait_recv()
        total = total + loss_all[step]
    loss_out[...] = total
    for unit in range(chunks + 1):
        add_second(unit)
    for step in range(1, N_DEV):
        loss_copy(step).wait_send()
    for unit in range(chunks + 1):
        for pair in range(4):
            core_copy(unit, pair).wait_send()
        first_copy(unit, 0).wait_send()
        first_copy(unit, 1).wait_send()
        second_copy(unit).wait_send()


def back_call(d_hnorm, x_rows, hid, gate, up, act, gain_mlp, gain_head, w_gate, w_up, w_down, row_id, head_grad, lse, picked, norm_rows, variant):
    groups, _, width = d_hnorm.shape
    slots, wide = gate.shape
    vocab = head_grad.shape[0]
    chunks = wide // WIDE_CHUNK
    units = chunks + 1
    f32, bf16 = jnp.float32, jnp.bfloat16
    dma = pltpu.SemaphoreType.DMA
    vmem = pl.BlockSpec(memory_space=pltpu.VMEM)
    hbm = pl.BlockSpec(memory_space=pl.ANY)
    piece_d = (wide // N_DEV, width)
    piece_w = (2, width // N_DEV, WIDE_CHUNK)
    return pl.pallas_call(
        functools.partial(back_kernel, groups),
        out_shape=(
            jax.ShapeDtypeStruct((8, 128), f32),
            jax.ShapeDtypeStruct((vocab, width), f32),
            jax.ShapeDtypeStruct((width // N_DEV, wide), f32),
            jax.ShapeDtypeStruct((width // N_DEV, wide), f32),
            jax.ShapeDtypeStruct(piece_d, f32),
        ),
        in_specs=[vmem, hbm, hbm, hbm, hbm, hbm, vmem, vmem, hbm, hbm, hbm, vmem, hbm, vmem, vmem, vmem],
        out_specs=(vmem,) * 5,
        scratch_shapes=[
            pltpu.VMEM((slots, width), bf16),
            pltpu.VMEM((slots, width), bf16),
            pltpu.VMEM((slots, wide), bf16),
            pltpu.VMEM((slots, wide), bf16),
            pltpu.VMEM((slots, wide), bf16),
            pltpu.VMEM((width, wide), bf16),
            pltpu.VMEM((width, wide), bf16),
            pltpu.VMEM((wide, width), bf16),
            pltpu.VMEM((slots, width), f32),
            pltpu.VMEM((slots, width), bf16),
            pltpu.VMEM((width, slots), bf16),
            pltpu.VMEM((width, slots), bf16),
            pltpu.VMEM((slots, width), f32),
            pltpu.VMEM((slots, WIDE_CHUNK), bf16),
            pltpu.VMEM((slots, WIDE_CHUNK), bf16),
            pltpu.VMEM((slots, 3 * width), bf16),
            pltpu.VMEM((N_DEV,) + piece_d, f32),
            pltpu.VMEM((4,) + piece_d, f32),
            pltpu.VMEM((2,) + piece_d, f32),
            pltpu.VMEM(piece_d, f32),
            pltpu.VMEM((chunks, N_DEV) + piece_w, f32),
            pltpu.VMEM((chunks, 4) + piece_w, f32),
            pltpu.VMEM((chunks, 2) + piece_w, f32),
            pltpu.VMEM((chunks,) + piece_w, f32),
            pltpu.VMEM((N_DEV, 8, 128), f32),
            pltpu.VMEM((8, 128), f32),
            dma((7,)),
            dma((2,)),
            dma((N_DEV,)),
            dma((N_DEV,)),
            dma((units, 4)),
            dma((units, 4)),
            dma((units, 2)),
            dma((units, 2)),
            dma((units,)),
            dma((units,)),
        ],
        compiler_params=pltpu.CompilerParams(collective_id=2 + 2 * variant, has_side_effects=True, vmem_limit_bytes=VMEM_MAX),
        cost_estimate=pl.CostEstimate(flops=16 * slots * wide * width, bytes_accessed=6 * slots * wide, transcendentals=slots * wide),
        name="back",
    )(d_hnorm, x_rows, hid, gate, up, act, gain_mlp.reshape(1, width), gain_head.reshape(1, width), w_gate, w_up, w_down, row_id, head_grad, lse, picked, norm_rows)


FEW_GROUPS, MANY_GROUPS = 6, 7


def solution(mesh):
    def swap(values, step):
        return lax.ppermute(values, "fsdp", [(dev, dev ^ step) for dev in range(N_DEV)])


    def device_step(tok_ids, tok_labels, loss_mask, table_shard, gain_mlp, gain_head, gate_shard, up_shard, down_shard):
        vocab, width = table_shard.shape
        vocab_all = vocab * N_DEV

        def row_part(mine):
            valid = mine != LAST_KEY
            row_id = jnp.where(valid, mine // vocab_all, 0)
            return row_id, jnp.where(valid, mine % vocab_all, -1), jnp.take(table_shard, row_id, axis=0)

        packed, info, table_t = gather_tokens(tok_ids, tok_labels, loss_mask, table_shard)
        own, packed = lax.optimization_barrier(((jnp.stack([gate_shard, up_shard]), down_shard), packed))
        even = [own] + [tuple(swap(block, step) for block in own) for step in (2, 4, 6)]
        many_slots = MANY_GROUPS * UNIT
        packed = jnp.sort(packed.reshape(-1))
        first = row_part(packed[:many_slots])
        even, first = lax.optimization_barrier((even, first))
        odd = [tuple(swap(block, 1) for block in slot) for slot in even]
        wide_slots, down_slots = zip(*[slot for two in zip(even, odd) for slot in two])
        most_load = info[2, 0].astype(jnp.int32)

        def one_round(groups, variant, rows):
            slots = groups * UNIT
            row_id, label, x_rows = rows[0][:slots], rows[1][:slots], rows[2]
            hid, gate, up, act, h_norm, gate_full, up_full, down_full = forward_call(wide_slots, down_slots, x_rows, gain_mlp, gain_head, groups)
            d_hnorm, head_grad, lse, picked = head_call(h_norm.reshape(groups, UNIT, width), label.reshape(groups, 1, UNIT), info, table_shard, table_t, groups, variant)
            return tuple(back_call(d_hnorm, x_rows, hid, gate, up, act, gain_mlp, gain_head, gate_full, up_full, down_full, row_id.reshape(groups, 1, UNIT), head_grad, lse, picked, info, variant))

        rounds = (most_load + many_slots - 1) // many_slots
        keys = jnp.concatenate([packed, jnp.full((-packed.shape[0] % many_slots,), LAST_KEY, jnp.int32)])

        def few():
            return one_round(FEW_GROUPS, 0, first)

        def many():
            return one_round(MANY_GROUPS, 1, first)

        def several():
            def step(state):
                extra = one_round(MANY_GROUPS, 1, row_part(lax.dynamic_slice(keys, (state[0] * many_slots,), (many_slots,))))
                return (state[0] + 1, tuple(old + new for old, new in zip(state[1], extra)))

            shapes = jax.eval_shape(many)
            zeros = tuple(jnp.zeros(shape.shape, shape.dtype) for shape in shapes)
            return lax.while_loop(lambda state: state[0] < rounds, step, (jnp.int32(0), zeros))[1]

        branch = (most_load > FEW_GROUPS * UNIT).astype(jnp.int32) + (rounds > 1).astype(jnp.int32)
        loss, g_table, g_gate, g_up, g_down = lax.switch(branch, [few, many, several])
        return (loss[0, 0], g_table, g_gate, g_up, g_down)

    row_spec = P("fsdp", None)
    tok_spec = P("fsdp")
    return jax.shard_map(device_step, mesh=mesh, in_specs=(tok_spec, tok_spec, tok_spec, row_spec, P(), P(), row_spec, row_spec, row_spec), out_specs=(P(), row_spec, row_spec, row_spec, row_spec), check_vma=False)
```

```python
import functools
import math

import jax
import jax.numpy as jnp
from jax import lax
from jax.experimental import pallas as pl
from jax.experimental.pallas import tpu as pltpu
from jax.sharding import PartitionSpec as P

NORM_EPS = 1e-6
ROW_CONTRACT = (((1,), (1,)), ((), ()))
TOK_CONTRACT = (((0,), (0,)), ((), ()))
MESH = pl.DeviceIdType.MESH
LOG2E = math.log2(math.e)
LN2 = math.log(2.0)
N_DEV = 8
UNIT = 256
V_CHUNK = 1024
VMEM_MAX = 67_043_328
LAST_KEY = 2**31 - 1
WIDE_CHUNK = 1024


def peer_of(me, step):
    core = (me % 2 + step % 2) % 2
    col = ((me // 2) % 2 + (step // 2) % 2) % 2
    row = (me // 4 + step // 4) % 2
    return row * 4 + col * 2 + core


def pair_xor(pair, other):
    return ((pair // 2 + other // 2) % 2) * 2 + (pair % 2 + other % 2) % 2


def meet_all(me):
    barrier = pltpu.get_barrier_semaphore()
    for step in range(1, N_DEV):
        pl.semaphore_signal(barrier, inc=1, device_id=(peer_of(me, step),), device_id_type=MESH)
    pl.semaphore_wait(barrier, N_DEV - 1)


def remote(src, dst, send_sem, recv_sem, target):
    return pltpu.make_async_remote_copy(src_ref=src, dst_ref=dst, send_sem=send_sem, recv_sem=recv_sem, device_id=(target,), device_id_type=MESH)


def tokens_kernel(ids_hbm, labels_hbm, mask_hbm, table_hbm, packed_ref, info_ref, table_t_ref, every, table_buf, local_sems, send_sems, recv_sems):
    me = lax.axis_index("fsdp")
    vocab = table_buf.shape[0]
    own = [pltpu.make_async_copy(src, every.at[which, 0], local_sems.at[which]) for which, src in enumerate((ids_hbm, labels_hbm, mask_hbm))]
    table_copy = pltpu.make_async_copy(table_hbm, table_buf, local_sems.at[3])
    for copy in own + [table_copy]:
        copy.start()
    meet_all(me)
    for copy in own:
        copy.wait()
    copies = []
    for step in range(1, N_DEV):
        copy = remote(every.at[:, 0], every.at[:, step], send_sems.at[step], recv_sems.at[step], peer_of(me, step))
        copy.start()
        copies.append(copy)
    table_copy.wait()

    @pl.loop(0, vocab // 512)
    def _(block):
        rows = pl.ds(pl.multiple_of(block * 512, 512), 512)
        table_t_ref[:, rows] = table_buf[rows, :].astype(jnp.float32).T.astype(jnp.bfloat16)

    for copy in copies:
        copy.wait()
    ids, labels, mask = every[0], every[1], every[2]
    local = ids - me * vocab
    mine = (local >= 0) & (local < vocab) & (mask != 0)
    packed_ref[...] = jnp.where(mine, local * (vocab * N_DEV) + labels, LAST_KEY)
    weight = mask.astype(jnp.float32)

    def total(rows):
        return jnp.sum(jnp.sum(jnp.sum(rows, axis=0), axis=0, keepdims=True), axis=1, keepdims=True)

    count = total(weight)
    load = jnp.zeros((1, 1), jnp.float32)
    for dev in range(N_DEV):
        here = (ids >= dev * vocab) & (ids < (dev + 1) * vocab)
        load = jnp.maximum(load, total(jnp.where(here, weight, 0.0)))
    info_ref[0:1, :] = jnp.broadcast_to(jnp.log2(count), (1, 128))
    info_ref[1:2, :] = jnp.broadcast_to(1.0 / count, (1, 128))
    info_ref[2:3, :] = jnp.broadcast_to(load, (1, 128))
    info_ref[3:8, :] = jnp.zeros((5, 128), jnp.float32)


def gather_tokens(ids, labels, mask, table):
    rows = (ids.shape[0] // 128, 128)
    vocab, width = table.shape
    dma = pltpu.SemaphoreType.DMA
    vmem = pl.BlockSpec(memory_space=pltpu.VMEM)
    hbm = pl.BlockSpec(memory_space=pl.ANY)
    return pl.pallas_call(
        tokens_kernel,
        out_shape=(
            jax.ShapeDtypeStruct((N_DEV,) + rows, jnp.int32),
            jax.ShapeDtypeStruct((8, 128), jnp.float32),
            jax.ShapeDtypeStruct((width, vocab), jnp.bfloat16),
        ),
        in_specs=[hbm] * 4,
        out_specs=(vmem,) * 3,
        scratch_shapes=[pltpu.VMEM((3, N_DEV) + rows, jnp.int32), pltpu.VMEM((vocab, width), jnp.bfloat16), dma((4,)), dma((N_DEV,)), dma((N_DEV,))],
        compiler_params=pltpu.CompilerParams(collective_id=0, has_side_effects=True),
        name="gather_tokens",
    )(ids.reshape(rows), labels.reshape(rows), mask.reshape(rows), table)


def head_kernel(groups, vocab, hn_hbm, lab_hbm, norm_ref, table_ref, table_t_ref, dhn_ref, dtable_ref, lse_ref, pick_ref,
                hn_all, lab_all, lse_mine, lse_all, part_own, part_out, part_in, sum_in, dhn_acc,
                local_sems, ag_send, ag_recv, fw_send, lab_send, lab_recv, st_send, st_recv, d2_send, d2_recv, rs_send, rs_recv):
    me = lax.axis_index("fsdp")
    chunks = vocab // V_CHUNK
    pair_rows = 2 * UNIT

    lab_copy = pltpu.make_async_copy(lab_hbm, lab_all.at[0], local_sems.at[0])
    lab_copy.start()
    hn_copy = pltpu.make_async_copy(hn_hbm, hn_all.at[:, 0], local_sems.at[1])
    hn_copy.start()
    meet_all(me)
    lab_copy.wait()

    def label_send(step):
        return remote(lab_all.at[0], lab_all.at[step], lab_send.at[step], lab_recv.at[step], peer_of(me, step))

    def own_send(step, group):
        return remote(hn_all.at[group, 0], hn_all.at[group, step], ag_send.at[step, group], ag_recv.at[step, group], peer_of(me, step))

    def forward(step, group):
        return remote(hn_all.at[group, step], hn_all.at[group, step + 1], fw_send.at[step, group], ag_recv.at[step + 1, group], peer_of(me, 1))

    def stat_send(step, group):
        return remote(lse_mine.at[group], lse_all.at[group, step], st_send.at[step, group], st_recv.at[step, group], peer_of(me, step))

    def part_send(group, pair):
        return remote(part_out.at[group, pair], part_in.at[group, pair], d2_send.at[group, pair], d2_recv.at[group, pair], peer_of(me, 1))

    def home_send(group, pair):
        return remote(part_own.at[group, pair], sum_in.at[group, pair], rs_send.at[group, pair], rs_recv.at[group, pair], peer_of(me, 2 * pair))

    hn_copy.wait()

    @pl.loop(0, groups)
    def _(group):
        for step in (1, 2, 4, 6):
            own_send(step, group).start()

    for step in range(1, N_DEV):
        label_send(step).start()
    dtable_ref[...] = jnp.zeros_like(dtable_ref)
    pick_ref[...] = jnp.zeros_like(pick_ref)

    def table_rows(chunk):
        return table_ref[pl.ds(pl.multiple_of(chunk * V_CHUNK, V_CHUNK), V_CHUNK), :]

    def tile_one(turn):
        away = (turn // groups + 3) // 4
        return (1 - away) * turn + away * ((turn + 2 * groups) // 3 - groups), away * (1 + (turn + 2 * groups) % 3)

    def tile_two(turn):
        own = turn // (3 * groups)
        return (1 - own) * (turn // 3) + own * (turn - 3 * groups), (1 - own) * (3 - turn % 3)

    @pl.loop(0, 4 * groups)
    def _(turn):
        group, pair = tile_one(turn)

        @pl.when((turn >= groups - 1) & (turn < 4 * groups - 1))
        def _():
            next_group, next_pair = tile_one(turn + 1)
            own_send(2 * next_pair, next_group).wait_recv()
            forward(2 * next_pair, next_group).start()

        @pl.when(turn < groups)
        def _():
            own_send(1, group).wait_recv()

        @pl.when(turn >= groups)
        def _():
            forward(2 * pair, group).wait_recv()

        tile = hn_all[group, pl.ds(2 * pair, 2)].reshape(pair_rows, 256)
        run_max = jnp.full((8, pair_rows), -jnp.inf, jnp.float32)
        run_sum = jnp.zeros((8, pair_rows), jnp.float32)
        for chunk in range(chunks):
            logits = lax.dot_general(table_rows(chunk), tile, ROW_CONTRACT, preferred_element_type=jnp.float32)
            logits = logits.reshape(V_CHUNK // 8, 8, pair_rows)
            new_max = jnp.maximum(run_max, jnp.max(logits, axis=0))
            new_scaled = new_max * LOG2E
            run_sum = run_sum * jnp.exp2(run_max * LOG2E - new_scaled) + jnp.sum(jnp.exp2(logits * LOG2E - new_scaled[None]), axis=0)
            run_max = new_max
        scaled = run_max * LOG2E
        top = jnp.max(scaled, axis=0, keepdims=True)
        total = jnp.sum(run_sum * jnp.exp2(scaled - top), axis=0, keepdims=True)
        lse_mine[group, pair] = top + jnp.log2(total)

        @pl.when((pair == 1) & (group > 0))
        def _():
            for step in range(1, N_DEV):
                stat_send(step, group - 1).start()

    for step in range(1, N_DEV):
        label_send(step).wait_recv()

    log2_n = norm_ref[0:1, :]
    log2_n = jnp.concatenate([log2_n] * (pair_rows // 128), axis=1)
    inv_n = norm_ref[1:2, :]
    inv_n = jnp.concatenate([inv_n] * (pair_rows // 128), axis=1)
    row_iota = lax.broadcasted_iota(jnp.int32, (V_CHUNK, pair_rows), 0)

    def finish_pair(group, pair):
        part_send(group, pair).wait_recv()
        part_own[group, pair] = part_own[group, pair] + part_in[group, pair]

    @pl.loop(0, 4 * groups)
    def _(turn):
        group, pair = tile_two(turn)

        @pl.when(turn == 0)
        def _():
            for step in range(1, N_DEV):
                stat_send(step, groups - 1).start()

        @pl.when(pair == 3)
        def _():
            for step in range(1, N_DEV):
                stat_send(step, group).wait_recv()

        low, high = [], []
        for step in range(N_DEV):
            source = lse_mine.at[group] if step == 0 else lse_all.at[group, step]
            row = source[pair_xor(pair, step // 2)]
            halves = [row[:, :UNIT], row[:, UNIT:]]
            low.append(halves[step % 2])
            high.append(halves[1 - step % 2])
        both = [jnp.concatenate(two, axis=1) for two in zip(low, high)]
        top = functools.reduce(jnp.maximum, both)
        lse = top + jnp.log2(sum(jnp.exp2(part - top) for part in both))
        label = jnp.concatenate([lab_all[2 * pair, group], lab_all[2 * pair + 1, group]], axis=1)
        valid = label >= 0
        shift = jnp.where(valid, lse + log2_n, 1e30)

        @pl.when(pair == 0)
        def _():
            lse_ref[group] = jnp.where(valid, lse, 0.0)[:, :UNIT]

        tile = hn_all[group, pl.ds(2 * pair, 2)].reshape(pair_rows, 256)
        local_label = label - me * vocab
        sub_row = lax.broadcasted_iota(jnp.int32, (8, pair_rows), 0)
        tile_row = jnp.where(local_label % 8 == sub_row, local_label // 8, -1)
        block_row = lax.broadcasted_iota(jnp.int32, (V_CHUNK // 8, 8, pair_rows), 0)
        picked = jnp.zeros((8, pair_rows), jnp.float32)
        for chunk in range(chunks):
            logits = lax.dot_general(table_rows(chunk), tile, ROW_CONTRACT, preferred_element_type=jnp.float32)
            logits = logits.reshape(V_CHUNK // 8, 8, pair_rows)
            is_label = block_row == (tile_row - chunk * (V_CHUNK // 8))[None]
            for row in range(V_CHUNK // 8):
                picked = jnp.where(is_label[row], logits[row], picked)
            prob = jnp.exp2(logits * LOG2E - shift[None])
            d_logits = jnp.where(is_label, prob - inv_n[None], prob).reshape(V_CHUNK, pair_rows).astype(jnp.bfloat16)
            rows = pl.ds(chunk * V_CHUNK, V_CHUNK)
            dtable_ref[rows, :] += jnp.dot(d_logits, tile, preferred_element_type=jnp.float32)
            d_part = jnp.dot(table_t_ref[:, rows], d_logits, preferred_element_type=jnp.float32)
            if chunk == 0:
                dhn_acc[...] = d_part
            else:
                dhn_acc[...] += d_part
        pick_ref[...] += picked
        part_own[group, pair] = dhn_acc[:, :UNIT]
        part_out[group, pair] = dhn_acc[:, UNIT:]

        @pl.when(turn >= 1)
        def _():
            part_send(*tile_two(turn - 1)).start()

        @pl.when(turn >= 2)
        def _():
            finish_pair(*tile_two(turn - 2))

        @pl.when((turn >= 3) & (turn < 3 * groups + 3))
        def _():
            home_send(*tile_two(turn - 3)).start()

    part_send(groups - 1, 0).start()
    finish_pair(groups - 2, 0)
    finish_pair(groups - 1, 0)

    @pl.loop(0, groups)
    def _(group):
        total = part_own[group, 0]
        for pair in (1, 2, 3):
            home_send(group, pair).wait_recv()
            total = total + sum_in[group, pair]
        dhn_ref[group] = total.T
        for step in (1, 2, 4, 6):
            own_send(step, group).wait_send()
        for step in (2, 4, 6):
            forward(step, group).wait_send()
        for step in range(1, N_DEV):
            stat_send(step, group).wait_send()
        for pair in range(4):
            part_send(group, pair).wait_send()
        for pair in (1, 2, 3):
            home_send(group, pair).wait_send()

    for step in range(1, N_DEV):
        label_send(step).wait_send()


def head_call(h_norm, labels, norm_rows, table, table_t, groups, variant=0):
    vocab = table.shape[0]
    dma = pltpu.SemaphoreType.DMA
    vmem = pl.BlockSpec(memory_space=pltpu.VMEM)
    hbm = pl.BlockSpec(memory_space=pl.ANY)
    f32, bf16 = jnp.float32, jnp.bfloat16
    tokens = N_DEV * groups * UNIT
    return pl.pallas_call(
        functools.partial(head_kernel, groups, vocab),
        out_shape=(
            jax.ShapeDtypeStruct((groups, UNIT, 256), f32),
            jax.ShapeDtypeStruct((vocab, 256), f32),
            jax.ShapeDtypeStruct((groups, 1, UNIT), f32),
            jax.ShapeDtypeStruct((8, 2 * UNIT), f32),
        ),
        in_specs=[hbm, hbm, vmem, vmem, vmem],
        out_specs=(vmem, vmem, vmem, vmem),
        scratch_shapes=[
            pltpu.VMEM((groups, N_DEV, UNIT, 256), bf16),
            pltpu.VMEM((N_DEV, groups, 1, UNIT), jnp.int32),
            pltpu.VMEM((groups, 4, 1, 2 * UNIT), f32),
            pltpu.VMEM((groups, N_DEV, 4, 1, 2 * UNIT), f32),
            pltpu.VMEM((groups, 4, 256, UNIT), f32),
            pltpu.VMEM((groups, 4, 256, UNIT), f32),
            pltpu.VMEM((groups, 4, 256, UNIT), f32),
            pltpu.VMEM((groups, 4, 256, UNIT), f32),
            pltpu.VMEM((256, 2 * UNIT), f32),
            dma((2,)),
            dma((N_DEV, groups)),
            dma((N_DEV, groups)),
            dma((N_DEV, groups)),
            dma((N_DEV,)),
            dma((N_DEV,)),
            dma((N_DEV, groups)),
            dma((N_DEV, groups)),
            dma((groups, 4)),
            dma((groups, 4)),
            dma((groups, 4)),
            dma((groups, 4)),
        ],
        compiler_params=pltpu.CompilerParams(collective_id=1 + 2 * variant, has_side_effects=True, vmem_limit_bytes=VMEM_MAX),
        cost_estimate=pl.CostEstimate(flops=8 * tokens * vocab * 256, bytes_accessed=16 * vocab * 256, transcendentals=2 * tokens * vocab),
        name="head",
    )(h_norm, labels, norm_rows, table, table_t)


def rms_scale(rows_wide, norm_gain):
    inv_rms = lax.rsqrt(jnp.mean(rows_wide * rows_wide, axis=-1, keepdims=True) + NORM_EPS)
    return (rows_wide * inv_rms * norm_gain).astype(jnp.bfloat16), inv_rms


def forward_kernel(*refs):
    wide_slots, down_slots = refs[:N_DEV], refs[N_DEV : 2 * N_DEV]
    x_ref, gain1_ref, gain2_ref, hid_ref, gate_ref, up_ref, act_ref, hn_ref, gate_hbm, up_hbm, down_hbm, w_gate, w_up, w_down, in_sems, out_sems = refs[2 * N_DEV :]
    f32, bf16 = jnp.float32, jnp.bfloat16
    me = lax.axis_index("fsdp")
    rows_w, rows_d = wide_slots[0].shape[1], down_slots[0].shape[0]
    outs = [pltpu.make_async_copy(src, dst, out_sems.at[i]) for i, (src, dst) in enumerate([(w_gate, gate_hbm), (w_up, up_hbm), (w_down, down_hbm)])]

    @pl.when(pl.program_id(0) == 0)
    def _():
        copies = []
        for step in range(N_DEV):
            dev = peer_of(me, step)
            copies.append(pltpu.make_async_copy(wide_slots[step].at[0], w_gate.at[pl.ds(dev * rows_w, rows_w)], in_sems.at[step, 0]))
            copies.append(pltpu.make_async_copy(wide_slots[step].at[1], w_up.at[pl.ds(dev * rows_w, rows_w)], in_sems.at[step, 1]))
            copies.append(pltpu.make_async_copy(down_slots[step], w_down.at[pl.ds(dev * rows_d, rows_d)], in_sems.at[step, 2]))
        for copy in copies:
            copy.start()
        for copy in copies:
            copy.wait()
        for copy in outs:
            copy.start()

    emb = x_ref[...].astype(f32)
    a_norm, _ = rms_scale(emb, gain1_ref[...])
    for chunk in range(w_gate.shape[1] // 512):
        cols = slice(chunk * 512, (chunk + 1) * 512)
        gate = jnp.dot(a_norm, w_gate[:, cols], preferred_element_type=f32).astype(bf16)
        up = jnp.dot(a_norm, w_up[:, cols], preferred_element_type=f32).astype(bf16)
        gate_ref[:, cols] = gate
        up_ref[:, cols] = up
        wide = gate.astype(f32)
        act_ref[:, cols] = (wide * jax.nn.sigmoid(wide) * up.astype(f32)).astype(bf16)
    hid = (emb + jnp.dot(act_ref[...], w_down[...], preferred_element_type=f32)).astype(bf16)
    hid_ref[...] = hid
    hn_ref[...], _ = rms_scale(hid.astype(f32), gain2_ref[...])

    @pl.when(pl.program_id(0) == pl.num_programs(0) - 1)
    def _():
        for copy in outs:
            copy.wait()


def forward_call(wide_slots, down_slots, x_rows, gain_mlp, gain_head, groups):
    slots, width = groups * UNIT, x_rows.shape[1]
    wide = wide_slots[0].shape[2]
    bf16 = jnp.bfloat16
    dma = pltpu.SemaphoreType.DMA
    hbm = pl.BlockSpec(memory_space=pl.ANY)
    gain = pl.BlockSpec((1, width), lambda i: (0, 0))
    narrow = pl.BlockSpec((UNIT, width), lambda i: (i, 0))
    broad = pl.BlockSpec((UNIT, wide), lambda i: (i, 0))
    full = [(width, wide), (width, wide), (wide, width)]
    return pl.pallas_call(
        forward_kernel,
        grid=(groups,),
        out_shape=[jax.ShapeDtypeStruct(shape, bf16) for shape in [(slots, width), (slots, wide), (slots, wide), (slots, wide), (slots, width)] + full],
        in_specs=[hbm] * (2 * N_DEV) + [narrow, gain, gain],
        out_specs=[narrow, broad, broad, broad, narrow, hbm, hbm, hbm],
        scratch_shapes=[pltpu.VMEM(shape, bf16) for shape in full] + [dma((N_DEV, 3)), dma((3,))],
        compiler_params=pltpu.CompilerParams(vmem_limit_bytes=VMEM_MAX),
        cost_estimate=pl.CostEstimate(flops=6 * slots * wide * width, bytes_accessed=6 * slots * wide, transcendentals=slots * wide),
        name="block_forward",
    )(*wide_slots, *down_slots, x_rows, gain_mlp.reshape(1, width), gain_head.reshape(1, width))


def back_kernel(groups, dhn_ref, x_hbm, hid_hbm, gate_hbm, up_hbm, act_hbm, gain1_ref, gain2_ref, w_gate_hbm, w_up_hbm, w_down_hbm, rows_ref, head_hbm, lse_ref, pick_ref, norm_ref,
                loss_out, dtable_ref, dgate_ref, dup_ref, ddown_ref,
                x_buf, hid_buf, gate_buf, up_buf, act_buf, w_gate, w_up, w_down, dh_wide, dh_narrow, dh_t, a_t, da_acc, dp_buf, dq_buf, dx_parts,
                down_acc, down_core, down_first, down_second, wide_acc, wide_core, wide_first, wide_second, loss_all, loss_ref,
                in_sems, tile_sems, loss_send, loss_recv, core_send, core_recv, first_send, first_recv, second_send, second_recv):
    me = lax.axis_index("fsdp")
    core = me % 2
    first_step = 2 + 2 * core
    second_step = 4 - 2 * core
    chunk_w = WIDE_CHUNK
    chunks = w_gate.shape[1] // chunk_w
    f32, bf16 = jnp.float32, jnp.bfloat16

    whole = [(x_hbm.at[pl.ds(0, groups * UNIT)], x_buf), (hid_hbm, hid_buf), (act_hbm, act_buf), (w_down_hbm, w_down), (w_gate_hbm, w_gate), (w_up_hbm, w_up), (head_hbm, dtable_ref)]
    loads = [pltpu.make_async_copy(src, dst, in_sems.at[i]) for i, (src, dst) in enumerate(whole)]
    tiles = [pltpu.make_async_copy(src, dst, tile_sems.at[i]) for i, (src, dst) in enumerate([(gate_hbm, gate_buf), (up_hbm, up_buf)])]
    for load in loads[:4] + tiles + loads[4:]:
        load.start()
    nats = jnp.sum(jnp.sum(lse_ref[...], axis=0), axis=1, keepdims=True) * LN2
    gold = jnp.sum(jnp.sum(pick_ref[...], axis=0, keepdims=True), axis=1, keepdims=True)
    loss_ref[...] = jnp.broadcast_to(nats - gold, (8, 128)) * norm_ref[1:2, :]
    meet_all(me)

    def loss_copy(step):
        return remote(loss_ref, loss_all.at[step], loss_send.at[step], loss_recv.at[step], peer_of(me, step))

    def piece(unit, step):
        if isinstance(unit, int) and unit == 0:
            return down_acc.at[peer_of(me, step)]
        return wide_acc.at[unit - 1, peer_of(me, step)]

    def core_copy(unit, pair):
        target = down_core.at[pair] if unit == 0 else wide_core.at[unit - 1, pair]
        return remote(piece(unit, 2 * pair + 1), target, core_send.at[unit, pair], core_recv.at[unit, pair], peer_of(me, 1))

    def first_copy(unit, which):
        target = down_first.at[which] if unit == 0 else wide_first.at[unit - 1, which]
        return remote(piece(unit, first_step if which == 0 else 6), target, first_send.at[unit, which], first_recv.at[unit, which], peer_of(me, first_step))

    def second_copy(unit):
        target = down_second if unit == 0 else wide_second.at[unit - 1]
        return remote(piece(unit, second_step), target, second_send.at[unit], second_recv.at[unit], peer_of(me, second_step))

    def send_core(unit):
        for pair in (1, 2, 3, 0):
            core_copy(unit, pair).start()

    def add_core(unit):
        for pair in (3, 2, 1, 0):
            core_copy(unit, pair).wait_recv()
            dst = piece(unit, 2 * pair)
            dst[...] = dst[...] + (down_core[pair] if unit == 0 else wide_core[unit - 1, pair])
        first_copy(unit, 1).start()
        first_copy(unit, 0).start()

    def add_first(unit):
        for which in (1, 0):
            first_copy(unit, which).wait_recv()
            dst = piece(unit, second_step if which == 1 else 0)
            dst[...] = dst[...] + (down_first[which] if unit == 0 else wide_first[unit - 1, which])
        second_copy(unit).start()

    def add_second(unit):
        second_copy(unit).wait_recv()
        if unit == 0:
            ddown_ref[...] = down_acc[me] + down_second[...]
        else:
            both = wide_acc[unit - 1, me] + wide_second[unit - 1]
            cols = slice((unit - 1) * chunk_w, unit * chunk_w)
            dgate_ref[:, cols] = both[0]
            dup_ref[:, cols] = both[1]

    loads[0].wait()
    loads[1].wait()

    @pl.loop(0, groups)
    def _(group):
        rows = pl.ds(pl.multiple_of(group * UNIT, UNIT), UNIT)
        hid = hid_buf[rows, :].astype(f32)
        inv_second = lax.rsqrt(jnp.mean(hid * hid, axis=-1, keepdims=True) + NORM_EPS)
        scaled = dhn_ref[group] * gain2_ref[...]
        d_hid = inv_second * (scaled - hid * (inv_second * inv_second) * jnp.mean(scaled * hid, axis=-1, keepdims=True))
        dh_wide[rows, :] = d_hid
        dh_narrow[rows, :] = d_hid.astype(bf16)
        dh_t[:, rows] = d_hid.astype(bf16).astype(f32).T.astype(bf16)
        emb = x_buf[rows, :].astype(f32)
        inv_first = lax.rsqrt(jnp.mean(emb * emb, axis=-1, keepdims=True) + NORM_EPS)
        a_norm = (emb * inv_first * gain1_ref[...]).astype(bf16)
        a_t[:, rows] = a_norm.astype(f32).T.astype(bf16)
        da_acc[rows, :] = jnp.zeros((UNIT, 256), f32)

    for step in range(1, N_DEV):
        loss_copy(step).start()
    loads[2].wait()

    @pl.loop(0, N_DEV)
    def _(dev):
        cols = pl.ds(pl.multiple_of(dev * 256, 256), 256)
        down_acc[dev] = jnp.dot(dh_t[...], act_buf[:, cols], preferred_element_type=f32).T

    send_core(0)
    loads[3].wait()
    for tile in tiles:
        tile.wait()
    loads[4].wait()
    loads[5].wait()
    for chunk in range(chunks):
        cols = slice(chunk * chunk_w, (chunk + 1) * chunk_w)

        @pl.loop(0, groups)
        def _(group):
            rows = pl.ds(pl.multiple_of(group * UNIT, UNIT), UNIT)
            d_act = lax.dot_general(dh_narrow[rows, :], w_down[cols, :], ROW_CONTRACT, preferred_element_type=f32)
            gate = gate_buf[rows, cols].astype(f32)
            up = up_buf[rows, cols].astype(f32)
            sig = jax.nn.sigmoid(gate)
            d_up = (d_act * gate * sig).astype(bf16)
            d_gate = (d_act * up * sig * (1.0 + gate * (1.0 - sig))).astype(bf16)
            dp_buf[rows, :] = d_gate
            dq_buf[rows, :] = d_up
            @pl.when(group == 2)
            def _():
                add_core(chunk)
                if chunk >= 1:
                    add_first(chunk - 1)

            da_acc[rows, :] += lax.dot_general(d_gate, w_gate[:, cols], ROW_CONTRACT, preferred_element_type=f32) + lax.dot_general(d_up, w_up[:, cols], ROW_CONTRACT, preferred_element_type=f32)

        grad_gate = jnp.dot(a_t[...], dp_buf[...], preferred_element_type=f32)
        wide_acc[chunk, :, 0] = grad_gate.reshape(N_DEV, 32, chunk_w)
        grad_up = jnp.dot(a_t[...], dq_buf[...], preferred_element_type=f32)
        wide_acc[chunk, :, 1] = grad_up.reshape(N_DEV, 32, chunk_w)
        send_core(chunk + 1)

    @pl.loop(0, groups)
    def _(group):
        rows = pl.ds(pl.multiple_of(group * UNIT, UNIT), UNIT)
        emb = x_buf[rows, :].astype(f32)
        inv_first = lax.rsqrt(jnp.mean(emb * emb, axis=-1, keepdims=True) + NORM_EPS)
        scaled = da_acc[rows, :] * gain1_ref[...]
        dx = dh_wide[rows, :] + inv_first * (scaled - emb * (inv_first * inv_first) * jnp.mean(scaled * emb, axis=-1, keepdims=True))
        high = dx.astype(bf16)
        rest = dx - high.astype(f32)
        middle = rest.astype(bf16)
        dx_parts[rows, 0:256] = high
        dx_parts[rows, 256:512] = middle
        dx_parts[rows, 512:768] = (rest - middle.astype(f32)).astype(bf16)

    add_core(chunks)
    add_first(chunks - 1)
    loads[6].wait()
    row_block = 512
    blocks = dtable_ref.shape[0] // row_block
    row_iota = lax.broadcasted_iota(jnp.int32, (row_block, UNIT), 0)

    def scatter_block(block):
        base = block * row_block
        rows = pl.ds(pl.multiple_of(base, row_block), row_block)
        picks = jnp.concatenate([jnp.where(row_iota == rows_ref[group] - base, 1.0, 0.0).astype(bf16) for group in range(groups)], axis=1)
        parts = jnp.dot(picks, dx_parts[...], preferred_element_type=f32)
        dtable_ref[rows, :] += (parts[:, 0:256] + (parts[:, 256:512] + parts[:, 512:768]))

    @pl.loop(0, blocks // 2)
    def _(block):
        scatter_block(block)

    add_first(chunks)

    @pl.loop(blocks // 2, blocks)
    def _(block):
        scatter_block(block)

    total = loss_ref[...]
    for step in range(1, N_DEV):
        loss_copy(step).wait_recv()
        total = total + loss_all[step]
    loss_out[...] = total
    for unit in range(chunks + 1):
        add_second(unit)
    for step in range(1, N_DEV):
        loss_copy(step).wait_send()
    for unit in range(chunks + 1):
        for pair in range(4):
            core_copy(unit, pair).wait_send()
        first_copy(unit, 0).wait_send()
        first_copy(unit, 1).wait_send()
        second_copy(unit).wait_send()


def back_call(d_hnorm, x_rows, hid, gate, up, act, gain_mlp, gain_head, w_gate, w_up, w_down, row_id, head_grad, lse, picked, norm_rows, variant):
    groups, _, width = d_hnorm.shape
    slots, wide = gate.shape
    vocab = head_grad.shape[0]
    chunks = wide // WIDE_CHUNK
    units = chunks + 1
    f32, bf16 = jnp.float32, jnp.bfloat16
    dma = pltpu.SemaphoreType.DMA
    vmem = pl.BlockSpec(memory_space=pltpu.VMEM)
    hbm = pl.BlockSpec(memory_space=pl.ANY)
    piece_d = (wide // N_DEV, width)
    piece_w = (2, width // N_DEV, WIDE_CHUNK)
    return pl.pallas_call(
        functools.partial(back_kernel, groups),
        out_shape=(
            jax.ShapeDtypeStruct((8, 128), f32),
            jax.ShapeDtypeStruct((vocab, width), f32),
            jax.ShapeDtypeStruct((width // N_DEV, wide), f32),
            jax.ShapeDtypeStruct((width // N_DEV, wide), f32),
            jax.ShapeDtypeStruct(piece_d, f32),
        ),
        in_specs=[vmem, hbm, hbm, hbm, hbm, hbm, vmem, vmem, hbm, hbm, hbm, vmem, hbm, vmem, vmem, vmem],
        out_specs=(vmem,) * 5,
        scratch_shapes=[
            pltpu.VMEM((slots, width), bf16),
            pltpu.VMEM((slots, width), bf16),
            pltpu.VMEM((slots, wide), bf16),
            pltpu.VMEM((slots, wide), bf16),
            pltpu.VMEM((slots, wide), bf16),
            pltpu.VMEM((width, wide), bf16),
            pltpu.VMEM((width, wide), bf16),
            pltpu.VMEM((wide, width), bf16),
            pltpu.VMEM((slots, width), f32),
            pltpu.VMEM((slots, width), bf16),
            pltpu.VMEM((width, slots), bf16),
            pltpu.VMEM((width, slots), bf16),
            pltpu.VMEM((slots, width), f32),
            pltpu.VMEM((slots, WIDE_CHUNK), bf16),
            pltpu.VMEM((slots, WIDE_CHUNK), bf16),
            pltpu.VMEM((slots, 3 * width), bf16),
            pltpu.VMEM((N_DEV,) + piece_d, f32),
            pltpu.VMEM((4,) + piece_d, f32),
            pltpu.VMEM((2,) + piece_d, f32),
            pltpu.VMEM(piece_d, f32),
            pltpu.VMEM((chunks, N_DEV) + piece_w, f32),
            pltpu.VMEM((chunks, 4) + piece_w, f32),
            pltpu.VMEM((chunks, 2) + piece_w, f32),
            pltpu.VMEM((chunks,) + piece_w, f32),
            pltpu.VMEM((N_DEV, 8, 128), f32),
            pltpu.VMEM((8, 128), f32),
            dma((7,)),
            dma((2,)),
            dma((N_DEV,)),
            dma((N_DEV,)),
            dma((units, 4)),
            dma((units, 4)),
            dma((units, 2)),
            dma((units, 2)),
            dma((units,)),
            dma((units,)),
        ],
        compiler_params=pltpu.CompilerParams(collective_id=2 + 2 * variant, has_side_effects=True, vmem_limit_bytes=VMEM_MAX),
        cost_estimate=pl.CostEstimate(flops=16 * slots * wide * width, bytes_accessed=6 * slots * wide, transcendentals=slots * wide),
        name="back",
    )(d_hnorm, x_rows, hid, gate, up, act, gain_mlp.reshape(1, width), gain_head.reshape(1, width), w_gate, w_up, w_down, row_id, head_grad, lse, picked, norm_rows)


FEW_GROUPS, MANY_GROUPS = 6, 7


def solution(mesh):
    def swap(values, step):
        return lax.ppermute(values, "fsdp", [(dev, dev ^ step) for dev in range(N_DEV)])


    def device_step(tok_ids, tok_labels, loss_mask, table_shard, gain_mlp, gain_head, gate_shard, up_shard, down_shard):
        vocab, width = table_shard.shape
        vocab_all = vocab * N_DEV

        def row_part(mine):
            valid = mine != LAST_KEY
            row_id = jnp.where(valid, mine // vocab_all, 0)
            return row_id, jnp.where(valid, mine % vocab_all, -1), jnp.take(table_shard, row_id, axis=0)

        packed, info, table_t = gather_tokens(tok_ids, tok_labels, loss_mask, table_shard)
        own, packed = lax.optimization_barrier(((jnp.stack([gate_shard, up_shard]), down_shard), packed))
        even = [own] + [tuple(swap(block, step) for block in own) for step in (2, 4, 6)]
        many_slots = MANY_GROUPS * UNIT
        packed = jnp.sort(packed.reshape(-1))
        first = row_part(packed[:many_slots])
        even, first = lax.optimization_barrier((even, first))
        odd = [tuple(swap(block, 1) for block in slot) for slot in even]
        wide_slots, down_slots = zip(*[slot for two in zip(even, odd) for slot in two])
        most_load = info[2, 0].astype(jnp.int32)

        def one_round(groups, variant, rows):
            slots = groups * UNIT
            row_id, label, x_rows = rows[0][:slots], rows[1][:slots], rows[2]
            hid, gate, up, act, h_norm, gate_full, up_full, down_full = forward_call(wide_slots, down_slots, x_rows, gain_mlp, gain_head, groups)
            d_hnorm, head_grad, lse, picked = head_call(h_norm.reshape(groups, UNIT, width), label.reshape(groups, 1, UNIT), info, table_shard, table_t, groups, variant)
            return tuple(back_call(d_hnorm, x_rows, hid, gate, up, act, gain_mlp, gain_head, gate_full, up_full, down_full, row_id.reshape(groups, 1, UNIT), head_grad, lse, picked, info, variant))

        rounds = (most_load + many_slots - 1) // many_slots
        keys = jnp.concatenate([packed, jnp.full((-packed.shape[0] % many_slots,), LAST_KEY, jnp.int32)])

        def few():
            return one_round(FEW_GROUPS, 0, first)

        def many():
            return one_round(MANY_GROUPS, 1, first)

        def several():
            def step(state):
                extra = one_round(MANY_GROUPS, 1, row_part(lax.dynamic_slice(keys, (state[0] * many_slots,), (many_slots,))))
                return (state[0] + 1, tuple(old + new for old, new in zip(state[1], extra)))

            shapes = jax.eval_shape(many)
            zeros = tuple(jnp.zeros(shape.shape, shape.dtype) for shape in shapes)
            return lax.while_loop(lambda state: state[0] < rounds, step, (jnp.int32(0), zeros))[1]

        branch = (most_load > FEW_GROUPS * UNIT).astype(jnp.int32) + (rounds > 1).astype(jnp.int32)
        loss, g_table, g_gate, g_up, g_down = lax.switch(branch, [few, many, several])
        return (loss[0, 0], g_table, g_gate, g_up, g_down)

    row_spec = P("fsdp", None)
    tok_spec = P("fsdp")
    return jax.shard_map(device_step, mesh=mesh, in_specs=(tok_spec, tok_spec, tok_spec, row_spec, P(), P(), row_spec, row_spec, row_spec), out_specs=(P(), row_spec, row_spec, row_spec, row_spec), check_vma=False)
```
